256 devices in a mesh: seq: 32 (over x, z_hi, core), ch: 8 (over z_lo, y).
Axes of the slice: x: 4, y: 4, z: 8 (z_hi: 4, z_lo: 2; z = z_hi * 2 + z_lo), core: 2. Of those that a mesh axis runs over, the one named last changes fastest.
Arguments:
- queries: bfloat16 [8192, 4096], P('seq', 'ch'), may hold values from -6 to 6
- key_in: bfloat16 [8192, 4096], P('seq', 'ch'), may hold values from -6 to 6
- value_in: bfloat16 [8192, 4096], P('seq', 'ch'), may hold values from -6 to 6
- filter_raw: bfloat16 [8192, 4096], P('seq', 'ch'), may hold values from -6 to 6
- skip_gain: float32 [4096], P('ch'), may hold values from -4 to 4
- out_weight: bfloat16 [4096, 4096], P('ch'), may hold values from -0.09375 to 0.09375
- cotangent: bfloat16 [8192, 4096], P('seq', 'ch'), may hold values from -6 to 6
Outputs:
- projected: bfloat16 [8192, 4096], P('seq', 'ch')
- grad_query: bfloat16 [8192, 4096], P('seq', 'ch')
- grad_key: bfloat16 [8192, 4096], P('seq', 'ch')
- grad_value: bfloat16 [8192, 4096], P('seq', 'ch')
- grad_filter: bfloat16 [8192, 4096], P('seq', 'ch')
The draws below stay inside these ranges and needn't reach their ends.
All inputs are finite; a program needn't handle non-finite values.
Results may differ from the reference program's by a relative error of at most 0.015.
Values may be sent and summed in bfloat16 or wider, within the bound.
No kernel may reach another device: no remote copies, remote signals or barrier semaphores. Data moves between devices by JAX's collectives and lax.ppermute only.
A program may use at most 128 MiB of HBM per device.

```python
import math
import jax
import jax.numpy as jnp
from jax import lax

WIDTH = 4096
SEQ = 8192


def shard_levels(rng, extent, pieces, low, top_value):
    factor_of = 1.0
    for position, parts in pieces:
        draws = jax.random.uniform(jax.random.fold_in(jax.random.fold_in(rng, 6), position), (parts,), jnp.float32, low / len(pieces), top_value / len(pieces))
        factor_of = factor_of * jnp.repeat(jnp.exp(draws), extent[position] // parts).reshape((-1,) + (1,) * (len(extent) - 1 - position))
    return factor_of


def gaussian(key, dims, scale, bound, pieces=(), dtype=jnp.bfloat16):
    factor_of = shard_levels(key, dims, pieces, -0.22, 0.18) if pieces else 1.0
    result = jax.random.normal(key, dims, jnp.float32) * scale * factor_of
    return jnp.minimum(jnp.maximum(result, -bound), bound).astype(dtype)


def setup_inputs(seed: int = 0) -> dict:
    keys = jax.random.split(jax.random.key(seed), 8)
    queries = gaussian(keys[0], (SEQ, WIDTH), 1.0, 6.0, ((0, 32), (1, 8)))
    key_in = gaussian(keys[1], (SEQ, WIDTH), 1.0, 6.0, ((0, 32), (1, 8)))
    value_in = gaussian(keys[2], (SEQ, WIDTH), 1.0, 6.0, ((0, 32), (1, 8)))
    filter_raw = gaussian(keys[3], (SEQ, WIDTH), 1.0, 6.0, ((0, 32), (1, 8)))
    skip_gain = gaussian(keys[4], (WIDTH,), 1.0, 4.0, ((0, 8),), jnp.float32)
    out_weight = gaussian(keys[5], (WIDTH, WIDTH), WIDTH ** -0.5, 0.09375, ((0, 8),))
    cotangent = gaussian(keys[6], (SEQ, WIDTH), 1.0, 6.0, ((0, 32), (1, 8)))
    return dict(queries=queries, key_in=key_in, value_in=value_in, filter_raw=filter_raw, skip_gain=skip_gain, out_weight=out_weight, cotangent=cotangent)


def spectral_group(arrays):
    product_kv, filter_raw, grad_conv = arrays
    length = 2 * SEQ
    z_freq = jnp.fft.rfft(product_kv, n=length, axis=0)
    h_freq = jnp.fft.rfft(filter_raw, n=length, axis=0)
    g_freq = jnp.fft.rfft(grad_conv, n=length, axis=0)
    forward_part = jnp.fft.irfft(h_freq * z_freq, n=length, axis=0)[:SEQ]
    backward_part = jnp.fft.irfft(jnp.conj(h_freq) * g_freq, n=length, axis=0)[:SEQ]
    filter_part = jnp.fft.irfft(jnp.conj(z_freq) * g_freq, n=length, axis=0)[:SEQ]
    return (forward_part, backward_part, filter_part)

def reference(queries, key_in, value_in, filter_raw, skip_gain, out_weight, cotangent):
    product_kv = (key_in.astype(jnp.float32) * value_in.astype(jnp.float32)).astype(jnp.bfloat16)
    grad_mixed = jnp.dot(cotangent, out_weight.T, preferred_element_type=jnp.float32)
    grad_conv = (grad_mixed * queries.astype(jnp.float32)).astype(jnp.bfloat16)
    group_width = math.gcd(WIDTH, 256)
    groups = WIDTH // group_width

    def to_groups(array):
        return array.astype(jnp.float32).reshape(SEQ, groups, group_width).transpose(1, 0, 2)

    def from_groups(array):
        return array.transpose(1, 0, 2).reshape(SEQ, WIDTH)
    results = lax.map(spectral_group, (to_groups(product_kv), to_groups(filter_raw), to_groups(grad_conv)))
    factor = 1.0 / math.sqrt(SEQ)
    forward_part = from_groups(results[0]) * factor
    backward_part = from_groups(results[1]) * factor
    filter_part = from_groups(results[2]) * factor
    skip_values = skip_gain.astype(jnp.float32)
    convolved = forward_part + skip_values * product_kv.astype(jnp.float32)
    gated_output = (queries.astype(jnp.float32) * convolved).astype(jnp.bfloat16)
    projected = jnp.dot(gated_output, out_weight, preferred_element_type=jnp.float32).astype(jnp.bfloat16)
    grad_query = (grad_mixed * convolved).astype(jnp.bfloat16)
    grad_product = backward_part + skip_values * grad_conv.astype(jnp.float32)
    grad_key = (grad_product * value_in.astype(jnp.float32)).astype(jnp.bfloat16)
    grad_value = (grad_product * key_in.astype(jnp.float32)).astype(jnp.bfloat16)
    grad_filter = filter_part.astype(jnp.bfloat16)
    return (projected, grad_query, grad_key, grad_value, grad_filter)
```

```python
import math

import jax
import jax.numpy as jnp
import numpy as np
from jax import lax
from jax.experimental import pallas as pl
from jax.experimental.pallas import tpu as pltpu
from jax.sharding import PartitionSpec as P

bf16 = jnp.bfloat16
f32 = jnp.float32
LANES = 128


def split(table):
    high = table.astype(bf16)
    low = (table - high.astype(np.float64)).astype(bf16)
    return np.asarray(high), np.asarray(low)


def tables(length, devices):
    points = 2 * length
    half = points // LANES // 2
    parts = half // devices
    rows = np.arange(half)
    j = parts * (rows % devices) + rows // devices
    k1 = np.arange(half) + 0.5
    lanes = np.arange(LANES)
    angle = 2.0 * np.pi / (2 * half) * np.outer(k1, j)
    first = np.concatenate([np.cos(angle), -np.sin(angle)], 0)
    last = np.concatenate([np.cos(angle.T), -np.sin(angle.T)], 1)
    turn = 2.0 * np.pi / points * np.outer(k1, lanes)
    factor = 2.0 / (points * math.sqrt(length))
    turns = np.stack([np.cos(turn), -np.sin(turn), np.cos(turn) * factor, np.sin(turn) * factor])
    phase = 2.0 * np.pi / LANES * (np.outer(lanes, lanes) % LANES)
    c, s = np.cos(phase), np.sin(phase)
    over = np.block([[c, -s], [s, c]])
    under = np.block([[c, s], [-s, c]])
    first_high, first_low = split(first)
    last_high, last_low = split(last)
    return (
        np.concatenate([first_high, first_low], 0),
        np.stack(split(over)),
        np.stack(split(under)),
        np.concatenate([last_high, last_low], 0),
        turns.astype(np.float32),
    )


def dot(a, b):
    return lax.dot_general(a, b, (((1,), (0,)), ((), ())), preferred_element_type=f32)


def halves(x):
    high = x.astype(bf16)
    return high, (x - high.astype(f32)).astype(bf16)


def forward(x, first, turns):
    half = turns.shape[1]
    both = dot(first, x)
    a = both[: 2 * half] + both[2 * half :]
    real, imag = a[:half], a[half:]
    return jnp.concatenate(
        [real * turns[0] - imag * turns[1], real * turns[1] + imag * turns[0]], 1
    )


def lanes_dot(x, table):
    high, low = halves(x)
    return dot(high, table[0]) + dot(low, table[0]) + dot(high, table[1])


def backward(b, last, turns):
    half = turns.shape[1]
    real, imag = b[:, :LANES], b[:, LANES:]
    d = jnp.concatenate([real * turns[2] - imag * turns[3], real * turns[3] + imag * turns[2]], 0)
    high, low = halves(d)
    rows = last.shape[0] // 2
    both = dot(last, high)
    return both[:rows] + both[rows:] + dot(last[:rows], low)


def rows_of(x):
    parts = x.shape[-1] // LANES
    return jnp.concatenate([x[:, p * LANES : (p + 1) * LANES] for p in range(parts)], 0)


def unrows(y, devices):
    return jnp.concatenate(
        [y[p * devices : (p + 1) * devices] for p in range(y.shape[0] // devices)], 1
    )


def product(a, b, conjugate):
    ar, ai = a[:, :LANES], a[:, LANES:]
    br, bi = b[:, :LANES], b[:, LANES:]
    if conjugate:
        return jnp.concatenate([ar * br + ai * bi, ar * bi - ai * br], 1)
    return jnp.concatenate([ar * br - ai * bi, ar * bi + ai * br], 1)


def prepare_body(key_ref, value_ref, filter_ref, out_ref, pkv_ref):
    peers, _, width, local_rows = out_ref.shape
    pkv = (key_ref[...].astype(f32) * value_ref[...].astype(f32)).astype(bf16)
    pkv_ref[...] = pkv
    out_ref[:, 0] = pkv.T.reshape(peers, width, local_rows)
    out_ref[:, 1] = filter_ref[...].T.reshape(peers, width, local_rows)


def conv_body(x_ref, first_ref, over_ref, under_ref, last_ref, turns_ref, out_ref, spec_ref, a_ref):
    width, devices = x_ref.shape[1:3]
    half = turns_ref.shape[1]
    for s in range(2):
        for c in range(width):
            a_ref[s, c] = forward(rows_of(x_ref[s, c]), first_ref[...], turns_ref)
    spectra = lanes_dot(a_ref[...].reshape(2 * width * half, 2 * LANES), over_ref)
    spec_ref[...] = spectra.reshape(spec_ref.shape)
    for c in range(width):
        a_ref[0, c] = product(spec_ref[1, c], spec_ref[0, c], False)
    b = lanes_dot(a_ref[0].reshape(width * half, 2 * LANES), under_ref)
    a_ref[1] = b.reshape(width, half, 2 * LANES)
    for c in range(width):
        y = backward(a_ref[1, c], last_ref[...], turns_ref)
        out_ref[c] = unrows(y.astype(bf16), devices)


def back_body(x_ref, spec_ref, first_ref, over_ref, under_ref, last_ref, turns_ref, out_ref, a_ref):
    width, devices = x_ref.shape[:2]
    half = turns_ref.shape[1]
    for c in range(width):
        a_ref[0, c] = forward(rows_of(x_ref[c]), first_ref[...], turns_ref)
    g = lanes_dot(a_ref[0].reshape(width * half, 2 * LANES), over_ref)
    a_ref[0] = g.reshape(width, half, 2 * LANES)
    for c in range(width):
        g_c = a_ref[0, c]
        a_ref[1, c] = product(spec_ref[0, c], g_c, True)
        a_ref[0, c] = product(spec_ref[1, c], g_c, True)
    b = lanes_dot(a_ref[...].reshape(2 * width * half, 2 * LANES), under_ref)
    a_ref[...] = b.reshape(a_ref.shape)
    for s in range(2):
        for c in range(width):
            y = backward(a_ref[s, c], last_ref[...], turns_ref)
            out_ref[s, c] = unrows(y.astype(bf16), devices)


def mixed_body(cot_ref, weight_ref, queries_ref, mixed_ref, conv_ref, sent_ref):
    step = pl.program_id(0)
    term = lax.dot_general(
        cot_ref[0], weight_ref[...], (((1,), (1,)), ((), ())), preferred_element_type=f32
    )

    @pl.when(step == 0)
    def _():
        mixed_ref[...] = term

    @pl.when(step > 0)
    def _():
        mixed_ref[...] += term

    @pl.when(step == pl.num_programs(0) - 1)
    def _():
        g = (mixed_ref[...] * queries_ref[...].astype(f32)).astype(bf16)
        conv_ref[...] = g
        sent_ref[...] = g.T.reshape(sent_ref.shape)


def gate_body(conv_ref, pkv_ref, skip_ref, queries_ref, weight_ref, out_ref, convolved_ref, gated_ref):
    @pl.when(pl.program_id(0) == 0)
    def _():
        local_rows = queries_ref.shape[0]
        conv = conv_ref[...].reshape(-1, local_rows).T.astype(f32)
        convolved = conv + skip_ref[...] * pkv_ref[...].astype(f32)
        convolved_ref[...] = convolved
        gated_ref[...] = (queries_ref[...].astype(f32) * convolved).astype(bf16)

    out_ref[0] = dot(gated_ref[...], weight_ref[...]).astype(bf16)


def finish_body(res_ref, conv_ref, skip_ref, key_ref, value_ref, gk_ref, gv_ref, gf_ref):
    local_rows = key_ref.shape[0]
    gf_ref[...] = res_ref[:, 1].reshape(-1, local_rows).T
    product_grad = res_ref[:, 0].reshape(-1, local_rows).T.astype(f32)
    product_grad = product_grad + skip_ref[...] * conv_ref[...].astype(f32)
    gk_ref[...] = (product_grad * value_ref[...].astype(f32)).astype(bf16)
    gv_ref[...] = (product_grad * key_ref[...].astype(f32)).astype(bf16)


def cost(flops, nbytes):
    return pl.CostEstimate(flops=flops, transcendentals=0, bytes_accessed=nbytes)


def to_all(x, axis):
    return lax.all_to_all(x, axis, split_axis=0, concat_axis=0, tiled=True)


def on_device(queries, key_in, value_in, filter_raw, skip_gain, out_weight, cotangent):
    local_rows, local_width = queries.shape
    seq_devices = lax.axis_size("seq")
    ch_devices = lax.axis_size("ch")
    length = local_rows * seq_devices
    width = local_width // seq_devices
    half = length // LANES
    shape = jax.ShapeDtypeStruct
    table = [jnp.asarray(t) for t in tables(length, seq_devices)]
    skip = skip_gain.reshape(1, local_width)
    message = (seq_devices, width, local_rows)

    copies = to_all(jnp.broadcast_to(cotangent, (ch_devices, *cotangent.shape)), "ch")

    sent, pkv = pl.pallas_call(
        prepare_body,
        out_shape=(shape((seq_devices, 2, width, local_rows), bf16), shape(queries.shape, bf16)),
        cost_estimate=cost(3 << 20, 2 << 20),
    )(key_in, value_in, filter_raw)
    signals = jnp.transpose(to_all(sent, "seq"), (1, 2, 0, 3))

    conv, spectra = pl.pallas_call(
        conv_body,
        out_shape=(
            shape((width, seq_devices, local_rows), bf16),
            shape((2, width, half, 2 * LANES), f32),
        ),
        scratch_shapes=[pltpu.VMEM((2, width, half, 2 * LANES), f32)],
        cost_estimate=cost(1 << 31, 4 << 20),
    )(signals, *table)

    whole = lambda dims: pl.BlockSpec(dims, lambda i: (0,) * len(dims))
    mixed, grad_conv, g_sent = pl.pallas_call(
        mixed_body,
        grid=(ch_devices,),
        in_specs=[
            pl.BlockSpec((1, local_rows, local_width), lambda i: (i, 0, 0)),
            pl.BlockSpec((local_width, local_width), lambda i: (0, i)),
            whole(queries.shape),
        ],
        out_specs=(whole(queries.shape), whole(queries.shape), whole(message)),
        out_shape=(shape(queries.shape, f32), shape(queries.shape, bf16), shape(message, bf16)),
        cost_estimate=cost(1 << 31, 8 << 20),
    )(copies, out_weight, queries)

    both = jnp.stack([jnp.transpose(conv, (1, 0, 2)), g_sent], 1)
    both = to_all(both, "seq")

    partial, convolved = pl.pallas_call(
        gate_body,
        grid=(ch_devices,),
        in_specs=[
            whole(message),
            whole(queries.shape),
            whole(skip.shape),
            whole(queries.shape),
            pl.BlockSpec((local_width, local_width), lambda i: (0, i)),
        ],
        out_specs=(
            pl.BlockSpec((1, local_rows, local_width), lambda i: (i, 0, 0)),
            whole(queries.shape),
        ),
        out_shape=(
            shape((ch_devices, local_rows, local_width), bf16),
            shape(queries.shape, f32),
        ),
        scratch_shapes=[pltpu.VMEM(queries.shape, bf16)],
        cost_estimate=cost(1 << 31, 8 << 20),
    )(both[:, 0], pkv, skip, queries, out_weight)
    terms = to_all(partial, "ch")

    results = pl.pallas_call(
        back_body,
        out_shape=shape((2, width, seq_devices, local_rows), bf16),
        scratch_shapes=[pltpu.VMEM((2, width, half, 2 * LANES), f32)],
        cost_estimate=cost(1 << 31, 4 << 20),
    )(jnp.transpose(both[:, 1], (1, 0, 2)), spectra, *table)
    results = to_all(jnp.transpose(results, (2, 0, 1, 3)), "seq")

    grad_query = (mixed * convolved).astype(bf16)
    grad_key, grad_value, grad_filter = pl.pallas_call(
        finish_body,
        out_shape=(shape(queries.shape, bf16),) * 3,
        cost_estimate=cost(3 << 20, 2 << 20),
    )(results, grad_conv, skip, key_in, value_in)
    projected = jnp.sum(terms.astype(f32), axis=0).astype(bf16)
    return (projected, grad_query, grad_key, grad_value, grad_filter)


def solution(mesh):
    placed = (
        P("seq", "ch"),
        P("seq", "ch"),
        P("seq", "ch"),
        P("seq", "ch"),
        P("ch"),
        P("ch", None),
        P("seq", "ch"),
    )
    return jax.shard_map(
        on_device,
        mesh=mesh,
        in_specs=placed,
        out_specs=(P("seq", "ch"),) * 5,
        check_vma=False,
    )
```

```python
import math

import jax
import jax.numpy as jnp
import numpy as np
from jax import lax
from jax.experimental import pallas as pl
from jax.experimental.pallas import tpu as pltpu
from jax.sharding import PartitionSpec as P

bf16 = jnp.bfloat16
f32 = jnp.float32
LANES = 128


def split(table):
    high = table.astype(bf16)
    low = (table - high.astype(np.float64)).astype(bf16)
    return np.asarray(high), np.asarray(low)


def tables(length, devices):
    points = 2 * length
    half = points // LANES // 2
    parts = half // devices
    rows = np.arange(half)
    j = parts * (rows % devices) + rows // devices
    k1 = np.arange(half) + 0.5
    lanes = np.arange(LANES)
    angle = 2.0 * np.pi / (2 * half) * np.outer(k1, j)
    first = np.concatenate([np.cos(angle), -np.sin(angle)], 0)
    last = np.concatenate([np.cos(angle.T), -np.sin(angle.T)], 1)
    turn = 2.0 * np.pi / points * np.outer(k1, lanes)
    factor = 2.0 / (points * math.sqrt(length))
    turns = np.stack([np.cos(turn), -np.sin(turn), np.cos(turn) * factor, np.sin(turn) * factor])
    phase = 2.0 * np.pi / LANES * (np.outer(lanes, lanes) % LANES)
    c, s = np.cos(phase), np.sin(phase)
    over = np.block([[c, -s], [s, c]])
    under = np.block([[c, s], [-s, c]])
    first_high, first_low = split(first)
    last_high, last_low = split(last)
    return (
        np.concatenate([first_high, first_low], 0),
        np.stack(split(over)),
        np.stack(split(under)),
        np.concatenate([last_high, last_low], 0),
        turns.astype(np.float32),
    )


def dot(a, b):
    return lax.dot_general(a, b, (((1,), (0,)), ((), ())), preferred_element_type=f32)


def halves(x):
    high = x.astype(bf16)
    return high, (x - high.astype(f32)).astype(bf16)


def forward(x, first, turns):
    half = turns.shape[1]
    both = dot(first, x)
    a = both[: 2 * half] + both[2 * half :]
    real, imag = a[:half], a[half:]
    return jnp.concatenate(
        [real * turns[0] - imag * turns[1], real * turns[1] + imag * turns[0]], 1
    )


def lanes_dot(x, table):
    high, low = halves(x)
    return dot(high, table[0]) + dot(low, table[0]) + dot(high, table[1])


def backward(b, last, turns):
    half = turns.shape[1]
    real, imag = b[:, :LANES], b[:, LANES:]
    d = jnp.concatenate([real * turns[2] - imag * turns[3], real * turns[3] + imag * turns[2]], 0)
    high, low = halves(d)
    rows = last.shape[0] // 2
    both = dot(last, high)
    return both[:rows] + both[rows:] + dot(last[:rows], low)


def product(a, b, conjugate):
    ar, ai = a[:, :LANES], a[:, LANES:]
    br, bi = b[:, :LANES], b[:, LANES:]
    if conjugate:
        return jnp.concatenate([ar * br + ai * bi, ar * bi - ai * br], 1)
    return jnp.concatenate([ar * br - ai * bi, ar * bi + ai * br], 1)


def prepare_body(key_ref, value_ref, filter_ref, out_ref, pkv_ref):
    peers, _, width, local_rows = out_ref.shape
    pkv = (key_ref[...].astype(f32) * value_ref[...].astype(f32)).astype(bf16)
    pkv_ref[...] = pkv
    out_ref[:, 0] = pkv.T.reshape(peers, width, local_rows)
    out_ref[:, 1] = filter_ref[...].T.reshape(peers, width, local_rows)


def spread(x, rows_ref):
    for p in range(rows_ref.shape[0]):
        part = x[:, :, p * LANES : (p + 1) * LANES]
        rows_ref[p] = part.astype(f32).reshape(rows_ref.shape[1:])


def gather(rows_ref, out_ref, s):
    for p in range(rows_ref.shape[0]):
        part = rows_ref[p].reshape(*out_ref.shape[:1], *out_ref.shape[-2:-1], LANES).astype(bf16)
        if s is None:
            out_ref[:, :, p * LANES : (p + 1) * LANES] = part
        else:
            out_ref[:, s, :, p * LANES : (p + 1) * LANES] = part


def channel(rows_ref, c, devices, width):
    parts = [rows_ref[p, pl.ds(c, devices, stride=width), :] for p in range(rows_ref.shape[0])]
    return jnp.concatenate(parts, 0).astype(bf16)


def put_channel(rows_ref, c, devices, width, y):
    for p in range(rows_ref.shape[0]):
        rows_ref[p, pl.ds(c, devices, stride=width), :] = y[p * devices : (p + 1) * devices]


def conv_body(x_ref, first_ref, over_ref, under_ref, last_ref, turns_ref, out_ref, spec_ref, a_ref, rows_ref):
    devices, _, width, _ = x_ref.shape
    half = turns_ref.shape[1]
    for s in range(2):
        spread(x_ref[:, s], rows_ref)
        for c in range(width):
            x = channel(rows_ref, c, devices, width)
            a_ref[s, c] = forward(x, first_ref[...], turns_ref)
    spectra = lanes_dot(a_ref[...].reshape(2 * width * half, 2 * LANES), over_ref)
    spec_ref[...] = spectra.reshape(spec_ref.shape)
    for c in range(width):
        a_ref[0, c] = product(spec_ref[1, c], spec_ref[0, c], False)
    b = lanes_dot(a_ref[0].reshape(width * half, 2 * LANES), under_ref)
    a_ref[1] = b.reshape(width, half, 2 * LANES)
    for c in range(width):
        y = backward(a_ref[1, c], last_ref[...], turns_ref)
        put_channel(rows_ref, c, devices, width, y)
    gather(rows_ref, out_ref, None)


def back_body(x_ref, spec_ref, first_ref, over_ref, under_ref, last_ref, turns_ref, out_ref, a_ref, rows_ref):
    devices, _, width, _ = x_ref.shape
    half = turns_ref.shape[1]
    spread(x_ref[:, 1], rows_ref)
    for c in range(width):
        x = channel(rows_ref, c, devices, width)
        a_ref[0, c] = forward(x, first_ref[...], turns_ref)
    g = lanes_dot(a_ref[0].reshape(width * half, 2 * LANES), over_ref)
    a_ref[0] = g.reshape(width, half, 2 * LANES)
    for c in range(width):
        g_c = a_ref[0, c]
        a_ref[1, c] = product(spec_ref[0, c], g_c, True)
        a_ref[0, c] = product(spec_ref[1, c], g_c, True)
    b = lanes_dot(a_ref[...].reshape(2 * width * half, 2 * LANES), under_ref)
    a_ref[...] = b.reshape(a_ref.shape)
    for s in range(2):
        for c in range(width):
            y = backward(a_ref[s, c], last_ref[...], turns_ref)
            put_channel(rows_ref, c, devices, width, y)
        gather(rows_ref, out_ref, s)


def columns(weight_ref, block, width):
    return weight_ref[:, pl.ds(pl.multiple_of(block * width, width), width)]


def mixed_terms(from_ref, weight_ref, parts):
    total = None
    for k, part in enumerate(parts):
        term = lax.dot_general(
            part[...],
            columns(weight_ref, from_ref[k], part.shape[1]),
            (((1,), (1,)), ((), ())),
            preferred_element_type=f32,
        )
        total = term if total is None else total + term
    return total


def mixed_body(from_ref, weight_ref, *refs):
    *parts, out_ref = refs
    out_ref[...] = mixed_terms(from_ref, weight_ref, parts)


def conv_grad_body(from_ref, weight_ref, before_ref, queries_ref, forward_ref, *refs):
    *parts, mixed_ref, conv_ref, sent_ref = refs
    mixed = before_ref[...] + mixed_terms(from_ref, weight_ref, parts)
    mixed_ref[...] = mixed
    g = (mixed * queries_ref[...].astype(f32)).astype(bf16)
    conv_ref[...] = g
    sent_ref[:, 0] = forward_ref[...]
    sent_ref[:, 1] = g.T.reshape(forward_ref.shape)


def project(to_ref, weight_ref, gated, out_refs):
    for k, out_ref in enumerate(out_refs):
        out_ref[...] = dot(gated, columns(weight_ref, to_ref[k], out_ref.shape[1])).astype(bf16)


def gate_body(to_ref, weight_ref, conv_ref, pkv_ref, skip_ref, queries_ref, convolved_ref, gated_ref, *out_refs):
    local_rows = queries_ref.shape[0]
    conv = conv_ref[:, 0].reshape(-1, local_rows).T.astype(f32)
    convolved = conv + skip_ref[...] * pkv_ref[...].astype(f32)
    convolved_ref[...] = convolved
    gated = (queries_ref[...].astype(f32) * convolved).astype(bf16)
    gated_ref[...] = gated
    project(to_ref, weight_ref, gated, out_refs)


def project_body(to_ref, weight_ref, gated_ref, *out_refs):
    project(to_ref, weight_ref, gated_ref[...], out_refs)


def finish_body(res_ref, conv_ref, skip_ref, key_ref, value_ref, gk_ref, gv_ref, gf_ref):
    local_rows = key_ref.shape[0]
    gf_ref[...] = res_ref[:, 1].reshape(-1, local_rows).T
    product_grad = res_ref[:, 0].reshape(-1, local_rows).T.astype(f32)
    product_grad = product_grad + skip_ref[...] * conv_ref[...].astype(f32)
    gk_ref[...] = (product_grad * value_ref[...].astype(f32)).astype(bf16)
    gv_ref[...] = (product_grad * key_ref[...].astype(f32)).astype(bf16)


def call(body, operands, results, scratch=(), flops=1 << 20, scalars=0, limit=16):
    vmem = pl.BlockSpec(memory_space=pltpu.VMEM)
    smem = pl.BlockSpec(memory_space=pltpu.SMEM)
    return pl.pallas_call(
        body,
        in_specs=[smem] * scalars + [vmem] * (len(operands) - scalars),
        out_specs=[vmem] * len(results),
        out_shape=[jax.ShapeDtypeStruct(dims, kind) for dims, kind in results],
        scratch_shapes=list(scratch),
        cost_estimate=pl.CostEstimate(flops=flops, transcendentals=0, bytes_accessed=4 << 20),
        compiler_params=pltpu.CompilerParams(vmem_limit_bytes=limit << 20),
    )(*operands)


def to_all(x, axis):
    return lax.all_to_all(x, axis, split_axis=0, concat_axis=0, tiled=True)


def on_device(queries, key_in, value_in, filter_raw, skip_gain, out_weight, cotangent):
    local_rows, local_width = queries.shape
    seq_devices = lax.axis_size("seq")
    ch_devices = lax.axis_size("ch")
    length = local_rows * seq_devices
    width = local_width // seq_devices
    half = length // LANES
    table = [jnp.asarray(t) for t in tables(length, seq_devices)]
    skip = skip_gain.reshape(1, local_width)
    message = (seq_devices, width, local_rows)
    pair = (seq_devices, 2, width, local_rows)
    flat = queries.shape
    near = ch_devices // 2
    work = [
        pltpu.VMEM((2, width, half, 2 * LANES), f32),
        pltpu.VMEM((local_rows // LANES, seq_devices * width, LANES), f32),
    ]

    def peer(index, flip, shift):
        far, place = index // near, index % near
        return (far + flip) % 2 * near + (place + shift) % near

    def move(x, flip, shift):
        pairs = [(i, peer(i, flip, shift)) for i in range(ch_devices)]
        return lax.ppermute(x, "ch", pairs)

    here = lax.axis_index("ch")
    hops = sorted(range(1, near), key=lambda d: -min(d, near - d))

    def blocks(flip, sign):
        places = [[peer(i, flip, sign * d) for d in [0] + hops] for i in range(ch_devices)]
        return jnp.asarray(places, jnp.int32)[here]

    came = [blocks(f, -1) for f in range(2)]
    goes = [blocks(f, 1) for f in range(2)]

    other = move(cotangent, 1, 0)
    own_parts = [cotangent] + [move(cotangent, 0, d) for d in hops]
    sent, pkv = call(
        prepare_body, (key_in, value_in, filter_raw), [(pair, bf16), (flat, bf16)]
    )
    signals = to_all(sent, "seq")
    other_parts = [other] + [move(other, 0, d) for d in hops]

    (mixed,) = call(
        mixed_body, (came[0], out_weight, *own_parts), [(flat, f32)], flops=1 << 30, scalars=1
    )
    conv, spectra = call(
        conv_body,
        (signals, *table),
        [(message, bf16), ((2, width, half, 2 * LANES), f32)],
        work,
        1 << 31,
    )
    mixed, grad_conv, both = call(
        conv_grad_body,
        (came[1], out_weight, mixed, queries, conv, *other_parts),
        [(flat, f32), (flat, bf16), (pair, bf16)],
        flops=1 << 30,
        scalars=1,
    )
    both = to_all(both, "seq")

    convolved, gated, *far_terms = call(
        gate_body,
        (goes[1], out_weight, both, pkv, skip, queries),
        [(flat, f32), (flat, bf16)] + [(flat, bf16)] * near,
        flops=1 << 30,
        scalars=1,
    )
    far_terms = [far_terms[0]] + [move(x, 0, d) for x, d in zip(far_terms[1:], hops)]
    near_terms = call(
        project_body,
        (goes[0], out_weight, gated),
        [(flat, bf16)] * near,
        flops=1 << 30,
        scalars=1,
    )
    near_terms = [near_terms[0]] + [move(x, 0, d) for x, d in zip(near_terms[1:], hops)]
    (results,) = call(back_body, (both, spectra, *table), [(pair, bf16)], work, 1 << 31)
    results = to_all(results, "seq")

    total = lambda terms: sum(x.astype(f32) for x in terms)
    across = move(total(far_terms).astype(bf16), 1, 0)
    grad_query = (mixed * convolved).astype(bf16)
    grad_key, grad_value, grad_filter = call(
        finish_body, (results, grad_conv, skip, key_in, value_in), [(flat, bf16)] * 3
    )
    projected = total(near_terms + [across]).astype(bf16)
    return (projected, grad_query, grad_key, grad_value, grad_filter)


def solution(mesh):
    placed = (
        P("seq", "ch"),
        P("seq", "ch"),
        P("seq", "ch"),
        P("seq", "ch"),
        P("ch"),
        P("ch", None),
        P("seq", "ch"),
    )
    return jax.shard_map(
        on_device,
        mesh=mesh,
        in_specs=placed,
        out_specs=(P("seq", "ch"),) * 5,
        check_vma=False,
    )
```

```python
import functools
import math

import jax
import jax.numpy as jnp
import numpy as np
from jax import lax
from jax.experimental import pallas as pl
from jax.experimental.pallas import tpu as pltpu
from jax.sharding import PartitionSpec as P


bf16 = jnp.bfloat16
f32 = jnp.float32
LANES = 128


def split(table):
    high = table.astype(bf16)
    low = (table - high.astype(np.float64)).astype(bf16)
    return np.asarray(high), np.asarray(low)


def tables(length, devices):
    points = 2 * length
    half = points // LANES // 2
    parts = half // devices
    rows = np.arange(half)
    j = parts * (rows % devices) + rows // devices
    k1 = np.arange(half) + 0.5
    lanes = np.arange(LANES)
    angle = 2.0 * np.pi / (2 * half) * np.outer(k1, j)
    first = np.concatenate([np.cos(angle), -np.sin(angle)], 0)
    last = np.concatenate([np.cos(angle.T), -np.sin(angle.T)], 1)
    turn = 2.0 * np.pi / points * np.outer(k1, lanes)
    factor = 2.0 / (points * math.sqrt(length))
    turns = np.stack([np.cos(turn), -np.sin(turn), np.cos(turn) * factor, np.sin(turn) * factor])
    phase = 2.0 * np.pi / LANES * (np.outer(lanes, lanes) % LANES)
    c, s = np.cos(phase), np.sin(phase)
    over = np.block([[c, -s], [s, c]])
    under = np.block([[c, s], [-s, c]])
    first_high, first_low = split(first)
    last_high, last_low = split(last)
    return (
        np.concatenate([first_high, first_low], 0),
        np.stack(split(over)),
        np.stack(split(under)),
        np.concatenate([last_high, last_low], 0),
        turns.astype(np.float32),
    )


def dot(a, b):
    return lax.dot_general(a, b, (((1,), (0,)), ((), ())), preferred_element_type=f32)


def halves(x):
    high = x.astype(bf16)
    return high, (x - high.astype(f32)).astype(bf16)


def forward(x, first, turns):
    half = turns.shape[1]
    both = dot(first, x)
    a = both[: 2 * half] + both[2 * half :]
    real, imag = a[:half], a[half:]
    return jnp.concatenate(
        [real * turns[0] - imag * turns[1], real * turns[1] + imag * turns[0]], 1
    )


def lanes_dot(x, table):
    high, low = halves(x)
    return dot(high, table[0]) + dot(low, table[0]) + dot(high, table[1])


def backward(b, last, turns):
    real, imag = b[:, :LANES], b[:, LANES:]
    d = jnp.concatenate([real * turns[2] - imag * turns[3], real * turns[3] + imag * turns[2]], 0)
    high, low = halves(d)
    rows = last.shape[0] // 2
    both = dot(last, high)
    return both[:rows] + both[rows:] + dot(last[:rows], low)


def product(a, b, conjugate):
    ar, ai = a[:, :LANES], a[:, LANES:]
    br, bi = b[:, :LANES], b[:, LANES:]
    if conjugate:
        return jnp.concatenate([ar * br + ai * bi, ar * bi - ai * br], 1)
    return jnp.concatenate([ar * br - ai * bi, ar * bi + ai * br], 1)


def fetch(pairs, sems):
    copies = [pltpu.make_async_copy(a, b, sems.at[i]) for i, (a, b) in enumerate(pairs)]
    for copy in copies:
        copy.start()
    return copies


def prepare_body(key_hbm, value_hbm, filter_hbm, out_ref, pkv_ref, key_ref, value_ref, filter_ref, sems):
    copies = fetch([(key_hbm, key_ref), (value_hbm, value_ref), (filter_hbm, filter_ref)], sems)
    peers, _, width, local_rows = out_ref.shape
    copies[0].wait()
    copies[1].wait()
    pkv = (key_ref[...].astype(f32) * value_ref[...].astype(f32)).astype(bf16)
    pkv_ref[...] = pkv
    out_ref[:, 0] = pkv.T.reshape(peers, width, local_rows)
    copies[2].wait()
    out_ref[:, 1] = filter_ref[...].T.reshape(peers, width, local_rows)


def spread(x, rows_ref):
    for p in range(rows_ref.shape[0]):
        part = x[:, :, p * LANES : (p + 1) * LANES]
        rows_ref[p] = part.astype(f32).reshape(rows_ref.shape[1:])


def gather(rows_ref, out_ref, s):
    for p in range(rows_ref.shape[0]):
        part = rows_ref[p].reshape(*out_ref.shape[:1], *out_ref.shape[-2:-1], LANES).astype(bf16)
        if s is None:
            out_ref[:, :, p * LANES : (p + 1) * LANES] = part
        else:
            out_ref[:, s, :, p * LANES : (p + 1) * LANES] = part


def channel(rows_ref, c, devices, width):
    parts = [rows_ref[p, pl.ds(c, devices, stride=width), :] for p in range(rows_ref.shape[0])]
    return jnp.concatenate(parts, 0).astype(bf16)


def put_channel(rows_ref, c, devices, width, y):
    for p in range(rows_ref.shape[0]):
        rows_ref[p, pl.ds(c, devices, stride=width), :] = y[p * devices : (p + 1) * devices]


def conv_body(
    x_ref, first_hbm, turns_hbm, over_hbm, under_hbm, last_hbm, out_ref, spec_ref,
    a_ref, rows_ref, first_ref, turns_ref, over_ref, under_ref, last_ref, sems,
):
    copies = fetch(
        [
            (first_hbm, first_ref),
            (turns_hbm, turns_ref),
            (over_hbm, over_ref),
            (under_hbm, under_ref),
            (last_hbm, last_ref),
        ],
        sems,
    )
    devices, _, width, _ = x_ref.shape
    half = turns_ref.shape[1]
    for s in range(2):
        spread(x_ref[:, s], rows_ref)
        if s == 0:
            copies[0].wait()
            copies[1].wait()
        for c in range(width):
            x = channel(rows_ref, c, devices, width)
            a_ref[s, c] = forward(x, first_ref[...], turns_ref)
    for copy in copies[2:]:
        copy.wait()
    spectra = lanes_dot(a_ref[...].reshape(2 * width * half, 2 * LANES), over_ref)
    spec_ref[...] = spectra.reshape(spec_ref.shape)
    for c in range(width):
        a_ref[0, c] = product(spec_ref[1, c], spec_ref[0, c], False)
    b = lanes_dot(a_ref[0].reshape(width * half, 2 * LANES), under_ref)
    a_ref[1] = b.reshape(width, half, 2 * LANES)
    for c in range(width):
        y = backward(a_ref[1, c], last_ref[...], turns_ref)
        put_channel(rows_ref, c, devices, width, y)
    gather(rows_ref, out_ref, None)


def back_body(
    x_ref, spec_ref, first_hbm, turns_hbm, over_hbm, under_hbm, last_hbm, out_ref,
    a_ref, rows_ref, first_ref, turns_ref, over_ref, under_ref, last_ref, sems,
):
    copies = fetch(
        [
            (first_hbm, first_ref),
            (turns_hbm, turns_ref),
            (over_hbm, over_ref),
            (under_hbm, under_ref),
            (last_hbm, last_ref),
        ],
        sems,
    )
    devices, _, width, _ = x_ref.shape
    half = turns_ref.shape[1]
    spread(x_ref[:, 1], rows_ref)
    copies[0].wait()
    copies[1].wait()
    for c in range(width):
        x = channel(rows_ref, c, devices, width)
        a_ref[0, c] = forward(x, first_ref[...], turns_ref)
    for copy in copies[2:]:
        copy.wait()
    g = lanes_dot(a_ref[0].reshape(width * half, 2 * LANES), over_ref)
    a_ref[0] = g.reshape(width, half, 2 * LANES)
    for c in range(width):
        g_c = a_ref[0, c]
        a_ref[1, c] = product(spec_ref[0, c], g_c, True)
        a_ref[0, c] = product(spec_ref[1, c], g_c, True)
    b = lanes_dot(a_ref[...].reshape(2 * width * half, 2 * LANES), under_ref)
    a_ref[...] = b.reshape(a_ref.shape)
    for s in range(2):
        for c in range(width):
            y = backward(a_ref[s, c], last_ref[...], turns_ref)
            put_channel(rows_ref, c, devices, width, y)
        gather(rows_ref, out_ref, s)


def peer(index, near, flip, shift):
    return (index // near + flip) % 2 * near + (index % near + shift) % near


def weight_pairs(weight_hbm, weight_ref, flip, signed_hops):
    here = lax.axis_index("ch")
    near = len(signed_hops)
    width = weight_ref.shape[2]
    pairs = []
    for k, d in enumerate(signed_hops):
        start = pl.multiple_of(peer(here, near, flip, d + near) * width, width)
        pairs.append((weight_hbm.at[:, pl.ds(start, width)], weight_ref.at[k]))
    return pairs


def mixed_terms(copies, weight_ref, parts):
    total = None
    for k, part in enumerate(parts):
        copies[k].wait()
        term = lax.dot_general(
            part[...], weight_ref[k], (((1,), (1,)), ((), ())), preferred_element_type=f32
        )
        total = term if total is None else total + term
    return total


def mixed_body(hops, weight_hbm, own_hbm, *refs):
    *parts, out_ref, own_ref, weight_ref, sems = refs
    pairs = [(own_hbm, own_ref)] + weight_pairs(weight_hbm, weight_ref, 0, [-d for d in hops])
    copies = fetch(pairs, sems)
    copies[0].wait()
    out_ref[...] = mixed_terms(copies[1:], weight_ref, [own_ref] + parts)


def conv_grad_body(hops, weight_hbm, queries_hbm, before_ref, forward_ref, *refs):
    *parts, mixed_ref, conv_ref, sent_ref, queries_ref, weight_ref, sems = refs
    pairs = weight_pairs(weight_hbm, weight_ref, 1, [-d for d in hops])
    copies = fetch(pairs + [(queries_hbm, queries_ref)], sems)
    sent_ref[:, 0] = forward_ref[...]
    mixed = before_ref[...] + mixed_terms(copies, weight_ref, parts)
    mixed_ref[...] = mixed
    copies[-1].wait()
    g = (mixed * queries_ref[...].astype(f32)).astype(bf16)
    conv_ref[...] = g
    sent_ref[:, 1] = g.T.reshape(forward_ref.shape)


def project(copies, weight_ref, gated, out_refs):
    for k, out_ref in enumerate(out_refs):
        copies[k].wait()
        out_ref[...] = dot(gated, weight_ref[k]).astype(bf16)


def gate_body(hops, weight_hbm, queries_hbm, conv_ref, pkv_ref, skip_ref, *refs):
    convolved_ref, gated_ref, *out_refs, queries_ref, weight_ref, sems = refs
    pairs = weight_pairs(weight_hbm, weight_ref, 1, hops)
    copies = fetch([(queries_hbm, queries_ref)] + pairs, sems)
    local_rows = queries_ref.shape[0]
    conv = conv_ref[:, 0].reshape(-1, local_rows).T.astype(f32)
    convolved = conv + skip_ref[...] * pkv_ref[...].astype(f32)
    convolved_ref[...] = convolved
    copies[0].wait()
    gated = (queries_ref[...].astype(f32) * convolved).astype(bf16)
    gated_ref[...] = gated
    project(copies[1:], weight_ref, gated, out_refs)


def project_body(hops, weight_hbm, gated_ref, *refs):
    *out_refs, weight_ref, sems = refs
    copies = fetch(weight_pairs(weight_hbm, weight_ref, 0, hops), sems)
    project(copies, weight_ref, gated_ref[...], out_refs)


def finish_body(res_ref, conv_ref, skip_ref, key_ref, value_ref, gk_ref, gv_ref, gf_ref):
    local_rows = key_ref.shape[0]
    gf_ref[...] = res_ref[:, 1].reshape(-1, local_rows).T
    product_grad = res_ref[:, 0].reshape(-1, local_rows).T.astype(f32)
    product_grad = product_grad + skip_ref[...] * conv_ref[...].astype(f32)
    gk_ref[...] = (product_grad * value_ref[...].astype(f32)).astype(bf16)
    gv_ref[...] = (product_grad * key_ref[...].astype(f32)).astype(bf16)


def call(body, operands, results, scratch=(), flops=1 << 20, hbm=(), copies=0, limit=16):
    vmem = pl.BlockSpec(memory_space=pltpu.VMEM)
    left = pl.BlockSpec(memory_space=pltpu.HBM)
    scratch = list(scratch)
    if copies:
        scratch.append(pltpu.SemaphoreType.DMA((copies,)))
    kernel = pl.pallas_call(
        body,
        in_specs=[left if i in hbm else vmem for i in range(len(operands))],
        out_specs=[vmem] * len(results),
        out_shape=[jax.ShapeDtypeStruct(dims, kind) for dims, kind in results],
        scratch_shapes=scratch,
        cost_estimate=pl.CostEstimate(flops=flops, transcendentals=0, bytes_accessed=4 << 20),
        compiler_params=pltpu.CompilerParams(vmem_limit_bytes=limit << 20),
    )
    stay = pltpu.with_memory_space_constraint
    return list(kernel(*(stay(x, pltpu.HBM) if i in hbm else x for i, x in enumerate(operands))))


def to_all(x, axis):
    return lax.all_to_all(x, axis, split_axis=0, concat_axis=0, tiled=True)


def step(queries, key_in, value_in, filter_raw, skip_gain, out_weight, cotangent):
    local_rows, local_width = queries.shape
    seq_devices = lax.axis_size("seq")
    ch_devices = lax.axis_size("ch")
    length = local_rows * seq_devices
    width = local_width // seq_devices
    half = length // LANES
    first, over, under, last, turns = [jnp.asarray(t) for t in tables(length, seq_devices)]
    table = (first, turns, over, under, last)
    skip = skip_gain.reshape(1, local_width)
    message = (seq_devices, width, local_rows)
    pair = (seq_devices, 2, width, local_rows)
    flat = queries.shape
    near = ch_devices // 2
    work = [
        pltpu.VMEM((2, width, half, 2 * LANES), f32),
        pltpu.VMEM((local_rows // LANES, seq_devices * width, LANES), f32),
    ] + [pltpu.VMEM(t.shape, t.dtype) for t in table]
    own = pltpu.VMEM(flat, bf16)
    weights = pltpu.VMEM((near, local_width, local_width), bf16)

    def move(x, flip, shift):
        pairs = [(i, peer(i, near, flip, shift)) for i in range(ch_devices)]
        return lax.ppermute(x, "ch", pairs)

    hops = sorted(range(1, near), key=lambda d: -min(d, near - d))
    places = [0] + hops
    body = lambda f: functools.partial(f, places)

    other = move(cotangent, 1, 0)
    own_parts = [move(cotangent, 0, d) for d in hops]
    sent, pkv = call(
        prepare_body,
        (key_in, value_in, filter_raw),
        [(pair, bf16), (flat, bf16)],
        [own] * 3,
        hbm=(0, 1, 2),
        copies=3,
    )
    signals = to_all(sent, "seq")
    other_parts = [other] + [move(other, 0, d) for d in hops]

    (mixed,) = call(
        body(mixed_body),
        (out_weight, cotangent, *own_parts),
        [(flat, f32)],
        [own, weights],
        1 << 30,
        hbm=(0, 1),
        copies=1 + near,
    )
    conv, spectra = call(
        conv_body,
        (signals, *table),
        [(message, bf16), ((2, width, half, 2 * LANES), f32)],
        work,
        1 << 31,
        hbm=range(1, 6),
        copies=5,
    )
    mixed, grad_conv, both = call(
        body(conv_grad_body),
        (out_weight, queries, mixed, conv, *other_parts),
        [(flat, f32), (flat, bf16), (pair, bf16)],
        [own, weights],
        1 << 30,
        hbm=(0, 1),
        copies=1 + near,
    )
    both = to_all(both, "seq")

    convolved, gated, *far_terms = call(
        body(gate_body),
        (out_weight, queries, both, pkv, skip),
        [(flat, f32), (flat, bf16)] + [(flat, bf16)] * near,
        [own, weights],
        1 << 30,
        hbm=(0, 1),
        copies=1 + near,
    )
    far_terms = far_terms[:1] + [move(x, 0, d) for x, d in zip(far_terms[1:], hops)]
    near_terms = call(
        body(project_body),
        (out_weight, gated),
        [(flat, bf16)] * near,
        [weights],
        1 << 30,
        hbm=(0,),
        copies=near,
    )
    near_terms = near_terms[:1] + [move(x, 0, d) for x, d in zip(near_terms[1:], hops)]
    (results,) = call(
        back_body,
        (both, spectra, *table),
        [(pair, bf16)],
        work,
        1 << 31,
        hbm=range(2, 7),
        copies=5,
    )
    results = to_all(results, "seq")

    total = lambda terms: sum(x.astype(f32) for x in terms)
    across = move(total(far_terms).astype(bf16), 1, 0)
    grad_query = (mixed * convolved).astype(bf16)
    grad_key, grad_value, grad_filter = call(
        finish_body, (results, grad_conv, skip, key_in, value_in), [(flat, bf16)] * 3
    )
    projected = total(near_terms + [across]).astype(bf16)
    return (projected, grad_query, grad_key, grad_value, grad_filter)


def solution(mesh):
    placed = (
        P("seq", "ch"),
        P("seq", "ch"),
        P("seq", "ch"),
        P("seq", "ch"),
        P("ch"),
        P("ch", None),
        P("seq", "ch"),
    )
    return jax.shard_map(
        step,
        mesh=mesh,
        in_specs=placed,
        out_specs=(P("seq", "ch"),) * 5,
        check_vma=False,
    )
```

```python
import functools
import math

import jax
import jax.numpy as jnp
import numpy as np
from jax import lax
from jax.experimental import pallas as pl
from jax.experimental.pallas import tpu as pltpu
from jax.sharding import PartitionSpec as P


bf16 = jnp.bfloat16
f32 = jnp.float32
LANES = 128


def split(table):
    high = table.astype(bf16)
    low = (table - high.astype(np.float64)).astype(bf16)
    return np.asarray(high), np.asarray(low)


def tables(length, devices):
    points = 2 * length
    half = points // LANES // 2
    parts = half // devices
    rows = np.arange(half)
    j = parts * (rows % devices) + rows // devices
    k1 = np.arange(half) + 0.5
    lanes = np.arange(LANES)
    angle = 2.0 * np.pi / (2 * half) * np.outer(k1, j)
    first = np.concatenate([np.cos(angle), -np.sin(angle)], 0)
    last = np.concatenate([np.cos(angle.T), -np.sin(angle.T)], 1)
    turn = 2.0 * np.pi / points * np.outer(k1, lanes)
    factor = 2.0 / (points * math.sqrt(length))
    turns = np.stack([np.cos(turn), -np.sin(turn), np.cos(turn) * factor, np.sin(turn) * factor])
    phase = 2.0 * np.pi / LANES * (np.outer(lanes, lanes) % LANES)
    c, s = np.cos(phase), np.sin(phase)
    over = np.block([[c, -s], [s, c]])
    under = np.block([[c, s], [-s, c]])
    first_high, first_low = split(first)
    last_high, last_low = split(last)
    return (
        np.concatenate([first_high, first_low], 0),
        over.astype(bf16),
        under.astype(bf16),
        np.concatenate([last_high, last_low], 0),
        turns.astype(np.float32),
    )


def dot(a, b):
    return lax.dot_general(a, b, (((1,), (0,)), ((), ())), preferred_element_type=f32)


def forward(x, first, turns):
    half = turns.shape[1]
    both = dot(first, x)
    a = both[: 2 * half] + both[2 * half :]
    real, imag = a[:half], a[half:]
    return jnp.concatenate(
        [real * turns[0] - imag * turns[1], real * turns[1] + imag * turns[0]], 1
    )


def lanes_dot(x, table):
    return dot(x.astype(bf16), table[...])


def backward(b, last, turns):
    real, imag = b[:, :LANES], b[:, LANES:]
    d = jnp.concatenate([real * turns[2] - imag * turns[3], real * turns[3] + imag * turns[2]], 0)
    rows = last.shape[0] // 2
    both = dot(last, d.astype(bf16))
    return both[:rows] + both[rows:]


def product(a, b, conjugate):
    ar, ai = a[:, :LANES], a[:, LANES:]
    br, bi = b[:, :LANES], b[:, LANES:]
    if conjugate:
        return jnp.concatenate([ar * br + ai * bi, ar * bi - ai * br], 1)
    return jnp.concatenate([ar * br - ai * bi, ar * bi + ai * br], 1)


def fetch(pairs, sems):
    copies = [pltpu.make_async_copy(a, b, sems.at[i]) for i, (a, b) in enumerate(pairs)]
    for copy in copies:
        copy.start()
    return copies


def prepare_body(key_hbm, value_hbm, filter_hbm, out_ref, pkv_ref, key_ref, value_ref, filter_ref, sems):
    copies = fetch([(key_hbm, key_ref), (value_hbm, value_ref), (filter_hbm, filter_ref)], sems)
    peers, _, width, local_rows = out_ref.shape
    copies[0].wait()
    copies[1].wait()
    pkv = (key_ref[...].astype(f32) * value_ref[...].astype(f32)).astype(bf16)
    pkv_ref[...] = pkv
    out_ref[:, 0] = pkv.T.reshape(peers, width, local_rows)
    copies[2].wait()
    out_ref[:, 1] = filter_ref[...].T.reshape(peers, width, local_rows)


def spread(x, rows_ref):
    for p in range(rows_ref.shape[0]):
        part = x[:, :, p * LANES : (p + 1) * LANES]
        rows_ref[p] = part.astype(f32).reshape(rows_ref.shape[1:])


def gather(rows_ref, out_ref, s):
    for p in range(rows_ref.shape[0]):
        part = rows_ref[p].reshape(*out_ref.shape[:1], *out_ref.shape[-2:-1], LANES).astype(bf16)
        if s is None:
            out_ref[:, :, p * LANES : (p + 1) * LANES] = part
        else:
            out_ref[:, s, :, p * LANES : (p + 1) * LANES] = part


def channel(rows_ref, c, devices, width):
    parts = [rows_ref[p, pl.ds(c, devices, stride=width), :] for p in range(rows_ref.shape[0])]
    return jnp.concatenate(parts, 0).astype(bf16)


def put_channel(rows_ref, c, devices, width, y):
    for p in range(rows_ref.shape[0]):
        rows_ref[p, pl.ds(c, devices, stride=width), :] = y[p * devices : (p + 1) * devices]


def conv_body(
    x_ref, first_ref, turns_ref, over_ref, under_hbm, last_hbm, weight_hbm, queries_hbm,
    out_ref, spec_ref, weight_ref, queries_ref, a_ref, rows_ref, under_ref, last_ref, sems,
):
    pairs = [(under_hbm, under_ref), (last_hbm, last_ref)]
    pairs += weight_pairs(weight_hbm, weight_ref, 1) + [(queries_hbm, queries_ref)]
    copies = fetch(pairs, sems)
    devices, _, width, _ = x_ref.shape
    half = turns_ref.shape[1]
    for s in range(2):
        spread(x_ref[:, s], rows_ref)
        for c in range(width):
            x = channel(rows_ref, c, devices, width)
            a_ref[s, c] = forward(x, first_ref[...], turns_ref)
    spectra = lanes_dot(a_ref[...].reshape(2 * width * half, 2 * LANES), over_ref)
    spec_ref[...] = spectra.reshape(spec_ref.shape)
    for c in range(width):
        a_ref[0, c] = product(spec_ref[1, c], spec_ref[0, c], False)
    copies[0].wait()
    copies[1].wait()
    b = lanes_dot(a_ref[0].reshape(width * half, 2 * LANES), under_ref)
    a_ref[1] = b.reshape(width, half, 2 * LANES)
    for c in range(width):
        y = backward(a_ref[1, c], last_ref[...], turns_ref)
        put_channel(rows_ref, c, devices, width, y)
    gather(rows_ref, out_ref, None)
    for copy in copies[2:]:
        copy.wait()


def back_body(
    x_ref, spec_ref, first_ref, turns_ref, over_ref, under_ref, last_ref, out_ref, a_ref, rows_ref
):
    devices, _, width, _ = x_ref.shape
    half = turns_ref.shape[1]
    spread(x_ref[:, 1], rows_ref)
    for c in range(width):
        x = channel(rows_ref, c, devices, width)
        a_ref[0, c] = forward(x, first_ref[...], turns_ref)
    g = lanes_dot(a_ref[0].reshape(width * half, 2 * LANES), over_ref)
    a_ref[0] = g.reshape(width, half, 2 * LANES)
    for c in range(width):
        g_c = a_ref[0, c]
        a_ref[1, c] = product(spec_ref[0, c], g_c, True)
        a_ref[0, c] = product(spec_ref[1, c], g_c, True)
    b = lanes_dot(a_ref[...].reshape(2 * width * half, 2 * LANES), under_ref)
    a_ref[...] = b.reshape(a_ref.shape)
    for s in range(2):
        for c in range(width):
            y = backward(a_ref[s, c], last_ref[...], turns_ref)
            put_channel(rows_ref, c, devices, width, y)
        gather(rows_ref, out_ref, s)


def peer(index, near, flip, shift):
    return (index // near + flip) % 2 * near + (index % near + shift) % near


def weight_pairs(weight_hbm, weight_ref, flip):
    here = lax.axis_index("ch")
    near, _, width = weight_ref.shape
    pairs = []
    for k in range(near):
        start = pl.multiple_of(peer(here, near, flip, k) * width, width)
        pairs.append((weight_hbm.at[:, pl.ds(start, width)], weight_ref.at[k]))
    return pairs


def mixed_term(part_ref, block):
    return lax.dot_general(
        part_ref[...], block, (((1,), (1,)), ((), ())), preferred_element_type=f32
    )


def mixed_body(hops, weight_hbm, own_hbm, *refs):
    near = len(hops)
    others = (len(refs) - near - 3) // 2
    parts = refs[: near - 1]
    others_hbm = refs[near - 1 : near - 1 + others]
    out_ref, *others_ref = refs[near - 1 + others : -3]
    own_ref, weight_ref, sems = refs[-3:]
    pairs = [(own_hbm, own_ref)] + weight_pairs(weight_hbm, weight_ref, 0)
    copies = fetch(pairs + list(zip(others_hbm, others_ref)), sems)
    for copy in copies[: 1 + near]:
        copy.wait()
    total = None
    for part_ref, d in zip((own_ref, *parts), hops):
        term = mixed_term(part_ref, weight_ref[-d % near])
        total = term if total is None else total + term
    out_ref[...] = total
    for copy in copies[1 + near :]:
        copy.wait()


def conv_grad_body(hops, weight_ref, queries_ref, before_ref, forward_ref, *refs):
    near = len(hops)
    others = (len(refs) - near - 4) // 2
    parts = refs[:near]
    others_hbm = refs[near : near + others]
    mixed_ref, conv_ref, sent_ref, *others_ref = refs[near + others : -1]
    copies = fetch(list(zip(others_hbm, others_ref)), refs[-1])
    sent_ref[:, 0] = forward_ref[...]
    mixed = before_ref[...]
    for part_ref, d in zip(parts, hops):
        mixed = mixed + mixed_term(part_ref, weight_ref[-d % near])
    mixed_ref[...] = mixed
    g = (mixed * queries_ref[...].astype(f32)).astype(bf16)
    conv_ref[...] = g
    sent_ref[:, 1] = g.T.reshape(forward_ref.shape)
    for copy in copies:
        copy.wait()


def gate_body(hops, weight_ref, queries_ref, conv_ref, pkv_ref, skip_ref, *refs):
    convolved_ref, gated_ref, *out_refs = refs
    local_rows = queries_ref.shape[0]
    conv = conv_ref[:, 0].reshape(-1, local_rows).T.astype(f32)
    convolved = conv + skip_ref[...] * pkv_ref[...].astype(f32)
    convolved_ref[...] = convolved
    gated = (queries_ref[...].astype(f32) * convolved).astype(bf16)
    gated_ref[...] = gated
    for out_ref, d in zip(out_refs, hops):
        out_ref[...] = dot(gated, weight_ref[d]).astype(bf16)


def project_body(hops, weight_hbm, gated_ref, *refs):
    *out_refs, weight_ref, sems = refs
    copies = fetch(weight_pairs(weight_hbm, weight_ref, 0), sems)
    for copy in copies:
        copy.wait()
    for out_ref, d in zip(out_refs, hops):
        out_ref[...] = dot(gated_ref[...], weight_ref[d]).astype(bf16)


def finish_body(res_ref, conv_ref, skip_ref, key_ref, value_ref, gk_ref, gv_ref, gf_ref):
    local_rows = key_ref.shape[0]
    gf_ref[...] = res_ref[:, 1].reshape(-1, local_rows).T
    product_grad = res_ref[:, 0].reshape(-1, local_rows).T.astype(f32)
    product_grad = product_grad + skip_ref[...] * conv_ref[...].astype(f32)
    gk_ref[...] = (product_grad * value_ref[...].astype(f32)).astype(bf16)
    gv_ref[...] = (product_grad * key_ref[...].astype(f32)).astype(bf16)


def call(body, operands, results, scratch=(), flops=1 << 20, hbm=(), copies=0, limit=16):
    vmem = pl.BlockSpec(memory_space=pltpu.VMEM)
    left = pl.BlockSpec(memory_space=pltpu.HBM)
    scratch = list(scratch)
    if copies:
        scratch.append(pltpu.SemaphoreType.DMA((copies,)))
    kernel = pl.pallas_call(
        body,
        in_specs=[left if i in hbm else vmem for i in range(len(operands))],
        out_specs=[vmem] * len(results),
        out_shape=[jax.ShapeDtypeStruct(dims, kind) for dims, kind in results],
        scratch_shapes=scratch,
        cost_estimate=pl.CostEstimate(flops=flops, transcendentals=0, bytes_accessed=4 << 20),
        compiler_params=pltpu.CompilerParams(vmem_limit_bytes=limit << 20),
    )
    stay = pltpu.with_memory_space_constraint
    return list(kernel(*(stay(x, pltpu.HBM) if i in hbm else x for i, x in enumerate(operands))))


def to_all(x, axis):
    return lax.all_to_all(x, axis, split_axis=0, concat_axis=0, tiled=True)


def step(queries, key_in, value_in, filter_raw, skip_gain, out_weight, cotangent):
    local_rows, local_width = queries.shape
    seq_devices = lax.axis_size("seq")
    ch_devices = lax.axis_size("ch")
    length = local_rows * seq_devices
    width = local_width // seq_devices
    half = length // LANES
    first, over, under, last, turns = [jnp.asarray(t) for t in tables(length, seq_devices)]
    table = (first, turns, over, under, last)
    skip = skip_gain.reshape(1, local_width)
    message = (seq_devices, width, local_rows)
    pair = (seq_devices, 2, width, local_rows)
    flat = queries.shape
    near = ch_devices // 2
    work = [
        pltpu.VMEM((2, width, half, 2 * LANES), f32),
        pltpu.VMEM((local_rows // LANES, seq_devices * width, LANES), f32),
    ]
    own = pltpu.VMEM(flat, bf16)
    blocks = (near, local_width, local_width)

    def move(x, flip, shift):
        pairs = [(i, peer(i, near, flip, shift)) for i in range(ch_devices)]
        return lax.ppermute(x, "ch", pairs)

    hops = sorted(range(1, near), key=lambda d: -min(d, near - d))
    places = [0] + hops
    body = lambda f: functools.partial(f, places)

    other = move(cotangent, 1, 0)
    own_parts = [move(cotangent, 0, d) for d in hops]
    sent, pkv = call(
        prepare_body,
        (key_in, value_in, filter_raw),
        [(pair, bf16), (flat, bf16)],
        [own] * 3,
        hbm=(0, 1, 2),
        copies=3,
    )
    signals = to_all(sent, "seq")
    other_parts = [other] + [move(other, 0, d) for d in hops]

    mixed, *first_table = call(
        body(mixed_body),
        (out_weight, cotangent, *own_parts, *table[:3]),
        [(flat, f32)] + [(t.shape, t.dtype) for t in table[:3]],
        [own, pltpu.VMEM(blocks, bf16)],
        1 << 30,
        hbm=(0, 1, *range(1 + near, 4 + near)),
        copies=4 + near,
    )
    conv, spectra, far_weight, own_queries = call(
        conv_body,
        (signals, *first_table, *table[3:], out_weight, queries),
        [
            (message, bf16),
            ((2, width, half, 2 * LANES), f32),
            (blocks, bf16),
            (flat, bf16),
        ],
        work + [pltpu.VMEM(t.shape, t.dtype) for t in table[3:]],
        1 << 31,
        hbm=(4, 5, 6, 7),
        copies=near + 3,
    )
    mixed, grad_conv, both, *last_table = call(
        body(conv_grad_body),
        (far_weight, own_queries, mixed, conv, *other_parts, *table),
        [(flat, f32), (flat, bf16), (pair, bf16)] + [(t.shape, t.dtype) for t in table],
        flops=1 << 30,
        hbm=range(4 + near, 4 + near + len(table)),
        copies=len(table),
    )
    both = to_all(both, "seq")

    convolved, gated, *far_terms = call(
        body(gate_body),
        (far_weight, own_queries, both, pkv, skip),
        [(flat, f32), (flat, bf16)] + [(flat, bf16)] * near,
        flops=1 << 30,
    )
    far_terms = far_terms[:1] + [move(x, 0, d) for x, d in zip(far_terms[1:], hops)]
    near_terms = call(
        body(project_body),
        (out_weight, gated),
        [(flat, bf16)] * near,
        [pltpu.VMEM(blocks, bf16)],
        1 << 30,
        hbm=(0,),
        copies=near,
    )
    near_terms = near_terms[:1] + [move(x, 0, d) for x, d in zip(near_terms[1:], hops)]
    (results,) = call(
        back_body,
        (both, spectra, *last_table),
        [(pair, bf16)],
        work,
        1 << 31,
    )
    results = to_all(results, "seq")

    total = lambda terms: sum(x.astype(f32) for x in terms)
    across = move(total(far_terms).astype(bf16), 1, 0)
    grad_query = (mixed * convolved).astype(bf16)
    grad_key, grad_value, grad_filter = call(
        finish_body, (results, grad_conv, skip, key_in, value_in), [(flat, bf16)] * 3
    )
    projected = total(near_terms + [across]).astype(bf16)
    return (projected, grad_query, grad_key, grad_value, grad_filter)


def solution(mesh):
    placed = (
        P("seq", "ch"),
        P("seq", "ch"),
        P("seq", "ch"),
        P("seq", "ch"),
        P("ch"),
        P("ch", None),
        P("seq", "ch"),
    )
    return jax.shard_map(
        step,
        mesh=mesh,
        in_specs=placed,
        out_specs=(P("seq", "ch"),) * 5,
        check_vma=False,
    )
```

```python
import functools
import math

import jax
import jax.numpy as jnp
import numpy as np
from jax import lax
from jax.experimental import pallas as pl
from jax.experimental.pallas import tpu as pltpu
from jax.sharding import PartitionSpec as P


bf16 = jnp.bfloat16
f32 = jnp.float32
LANES = 128


def split(table):
    high = table.astype(bf16)
    low = (table - high.astype(np.float64)).astype(bf16)
    return np.asarray(high), np.asarray(low)


def tables(length, devices):
    points = 2 * length
    half = points // LANES // 2
    parts = half // devices
    rows = np.arange(half)
    j = parts * (rows % devices) + rows // devices
    k1 = np.arange(half) + 0.5
    lanes = np.arange(LANES)
    angle = 2.0 * np.pi / (2 * half) * np.outer(k1, j)
    first = np.concatenate([np.cos(angle), -np.sin(angle)], 0)
    last = np.concatenate([np.cos(angle.T), -np.sin(angle.T)], 1)
    turn = 2.0 * np.pi / points * np.outer(k1, lanes)
    factor = 2.0 / (points * math.sqrt(length))
    turns = np.stack([np.cos(turn), -np.sin(turn), np.cos(turn) * factor, np.sin(turn) * factor])
    phase = 2.0 * np.pi / LANES * (np.outer(lanes, lanes) % LANES)
    c, s = np.cos(phase), np.sin(phase)
    over = np.block([[c, -s], [s, c]])
    under = np.block([[c, s], [-s, c]])
    first_high, first_low = split(first)
    last_high, last_low = split(last)
    return (
        np.concatenate([first_high, first_low], 0),
        over.astype(bf16),
        under.astype(bf16),
        np.concatenate([last_high, last_low], 0),
        turns.astype(np.float32),
    )


def dot(a, b):
    return lax.dot_general(a, b, (((1,), (0,)), ((), ())), preferred_element_type=f32)


def forward(signals, first, turns):
    half = turns.shape[1]
    both = dot(first, jnp.concatenate(signals, 1))
    a = both[: 2 * half] + both[2 * half :]
    rotated = []
    for k in range(len(signals)):
        real = a[:half, k * LANES : (k + 1) * LANES]
        imag = a[half:, k * LANES : (k + 1) * LANES]
        pair = [real * turns[0] - imag * turns[1], real * turns[1] + imag * turns[0]]
        rotated.append(jnp.concatenate(pair, 1))
    return rotated


def lanes_dot(x, table):
    return dot(x.astype(bf16), table[...])


def backward(spectra, last, turns):
    turned = []
    for b in spectra:
        real, imag = b[:, :LANES], b[:, LANES:]
        pair = [real * turns[2] - imag * turns[3], real * turns[3] + imag * turns[2]]
        turned.append(jnp.concatenate(pair, 0).astype(bf16))
    rows = last.shape[0] // 2
    both = dot(last, jnp.concatenate(turned, 1))
    y = both[:rows] + both[rows:]
    return [y[:, k * LANES : (k + 1) * LANES] for k in range(len(spectra))]


def product(a, b, conjugate):
    ar, ai = a[:, :LANES], a[:, LANES:]
    br, bi = b[:, :LANES], b[:, LANES:]
    if conjugate:
        return jnp.concatenate([ar * br + ai * bi, ar * bi - ai * br], 1)
    return jnp.concatenate([ar * br - ai * bi, ar * bi + ai * br], 1)


def fetch(pairs, sems):
    copies = [pltpu.make_async_copy(a, b, sems.at[i]) for i, (a, b) in enumerate(pairs)]
    for copy in copies:
        copy.start()
    return copies


def prepare_body(key_hbm, value_hbm, filter_hbm, out_ref, pkv_ref, key_ref, value_ref, filter_ref, sems):
    copies = fetch([(key_hbm, key_ref), (value_hbm, value_ref), (filter_hbm, filter_ref)], sems)
    peers, _, width, local_rows = out_ref.shape
    copies[0].wait()
    copies[1].wait()
    pkv = (key_ref[...].astype(f32) * value_ref[...].astype(f32)).astype(bf16)
    pkv_ref[...] = pkv
    out_ref[:, 0] = pkv.T.reshape(peers, width, local_rows)
    copies[2].wait()
    out_ref[:, 1] = filter_ref[...].T.reshape(peers, width, local_rows)


def spread(x, rows_ref):
    for p in range(rows_ref.shape[0]):
        part = x[:, :, p * LANES : (p + 1) * LANES]
        rows_ref[p] = part.astype(f32).reshape(rows_ref.shape[1:])


def gather(rows_ref, out_ref, s):
    for p in range(rows_ref.shape[0]):
        part = rows_ref[p].reshape(*out_ref.shape[:1], *out_ref.shape[-2:-1], LANES).astype(bf16)
        if s is None:
            out_ref[:, :, p * LANES : (p + 1) * LANES] = part
        else:
            out_ref[:, s, :, p * LANES : (p + 1) * LANES] = part


def channel(rows_ref, c, devices, width):
    parts = [rows_ref[p, pl.ds(c, devices, stride=width), :] for p in range(rows_ref.shape[0])]
    return jnp.concatenate(parts, 0).astype(bf16)


def put_channel(rows_ref, c, devices, width, y):
    for p in range(rows_ref.shape[0]):
        rows_ref[p, pl.ds(c, devices, stride=width), :] = y[p * devices : (p + 1) * devices]


def conv_body(
    x_ref, first_ref, turns_ref, over_ref, under_hbm, last_hbm, weight_hbm, queries_hbm,
    out_ref, spec_ref, weight_ref, queries_ref, a_ref, rows_ref, under_ref, last_ref, sems,
):
    pairs = [(under_hbm, under_ref), (last_hbm, last_ref)]
    pairs += weight_pairs(weight_hbm, weight_ref, 1) + [(queries_hbm, queries_ref)]
    copies = fetch(pairs, sems)
    devices, _, width, _ = x_ref.shape
    half = turns_ref.shape[1]
    for s in range(2):
        spread(x_ref[:, s], rows_ref)
        for c in range(0, width, 2):
            x = [channel(rows_ref, c + k, devices, width) for k in range(2)]
            a_ref[s, c], a_ref[s, c + 1] = forward(x, first_ref[...], turns_ref)
    spectra = lanes_dot(a_ref[...].reshape(2 * width * half, 2 * LANES), over_ref)
    spec_ref[...] = spectra.reshape(spec_ref.shape)
    for c in range(width):
        a_ref[0, c] = product(spec_ref[1, c], spec_ref[0, c], False)
    copies[0].wait()
    copies[1].wait()
    b = lanes_dot(a_ref[0].reshape(width * half, 2 * LANES), under_ref)
    a_ref[1] = b.reshape(width, half, 2 * LANES)
    for c in range(0, width, 2):
        y = backward([a_ref[1, c], a_ref[1, c + 1]], last_ref[...], turns_ref)
        for k in range(2):
            put_channel(rows_ref, c + k, devices, width, y[k])
    gather(rows_ref, out_ref, None)
    for copy in copies[2:]:
        copy.wait()


def back_body(
    x_ref, spec_ref, first_ref, turns_ref, over_ref, under_ref, last_ref, out_ref, a_ref, rows_ref
):
    devices, _, width, _ = x_ref.shape
    half = turns_ref.shape[1]
    spread(x_ref[:, 1], rows_ref)
    for c in range(0, width, 2):
        x = [channel(rows_ref, c + k, devices, width) for k in range(2)]
        a_ref[0, c], a_ref[0, c + 1] = forward(x, first_ref[...], turns_ref)
    g = lanes_dot(a_ref[0].reshape(width * half, 2 * LANES), over_ref)
    a_ref[0] = g.reshape(width, half, 2 * LANES)
    for c in range(width):
        g_c = a_ref[0, c]
        a_ref[1, c] = product(spec_ref[0, c], g_c, True)
        a_ref[0, c] = product(spec_ref[1, c], g_c, True)
    b = lanes_dot(a_ref[...].reshape(2 * width * half, 2 * LANES), under_ref)
    a_ref[...] = b.reshape(a_ref.shape)
    for s in range(2):
        for c in range(0, width, 2):
            y = backward([a_ref[s, c], a_ref[s, c + 1]], last_ref[...], turns_ref)
            for k in range(2):
                put_channel(rows_ref, c + k, devices, width, y[k])
        gather(rows_ref, out_ref, s)


def peer(index, near, flip, shift):
    return (index // near + flip) % 2 * near + (index % near + shift) % near


def weight_pairs(weight_hbm, weight_ref, flip):
    here = lax.axis_index("ch")
    near, _, width = weight_ref.shape
    pairs = []
    for k in range(near):
        start = pl.multiple_of(peer(here, near, flip, k) * width, width)
        pairs.append((weight_hbm.at[:, pl.ds(start, width)], weight_ref.at[k]))
    return pairs


def mixed_term(part_ref, block):
    return lax.dot_general(
        part_ref[...], block, (((1,), (1,)), ((), ())), preferred_element_type=f32
    )


def mixed_body(hops, weight_hbm, own_hbm, *refs):
    near = len(hops)
    others = (len(refs) - near - 3) // 2
    parts = refs[: near - 1]
    others_hbm = refs[near - 1 : near - 1 + others]
    out_ref, *others_ref = refs[near - 1 + others : -3]
    own_ref, weight_ref, sems = refs[-3:]
    pairs = [(own_hbm, own_ref)] + weight_pairs(weight_hbm, weight_ref, 0)
    copies = fetch(pairs + list(zip(others_hbm, others_ref)), sems)
    for copy in copies[: 1 + near]:
        copy.wait()
    total = None
    for part_ref, d in zip((own_ref, *parts), hops):
        term = mixed_term(part_ref, weight_ref[-d % near])
        total = term if total is None else total + term
    out_ref[...] = total
    for copy in copies[1 + near :]:
        copy.wait()


def conv_grad_body(hops, weight_ref, queries_ref, before_ref, forward_ref, *refs):
    near = len(hops)
    others = (len(refs) - near - 4) // 2
    parts = refs[:near]
    others_hbm = refs[near : near + others]
    mixed_ref, conv_ref, sent_ref, *others_ref = refs[near + others : -1]
    copies = fetch(list(zip(others_hbm, others_ref)), refs[-1])
    sent_ref[:, 0] = forward_ref[...]
    mixed = before_ref[...]
    for part_ref, d in zip(parts, hops):
        mixed = mixed + mixed_term(part_ref, weight_ref[-d % near])
    mixed_ref[...] = mixed
    g = (mixed * queries_ref[...].astype(f32)).astype(bf16)
    conv_ref[...] = g
    sent_ref[:, 1] = g.T.reshape(forward_ref.shape)
    for copy in copies:
        copy.wait()


def gate_body(hops, weight_ref, queries_ref, conv_ref, pkv_ref, skip_ref, *refs):
    convolved_ref, gated_ref, *out_refs = refs
    local_rows = queries_ref.shape[0]
    conv = conv_ref[:, 0].reshape(-1, local_rows).T.astype(f32)
    convolved = conv + skip_ref[...] * pkv_ref[...].astype(f32)
    convolved_ref[...] = convolved
    gated = (queries_ref[...].astype(f32) * convolved).astype(bf16)
    gated_ref[...] = gated
    for out_ref, d in zip(out_refs, hops):
        out_ref[...] = dot(gated, weight_ref[d]).astype(bf16)


def project_body(hops, weight_hbm, gated_ref, *refs):
    *out_refs, weight_ref, sems = refs
    copies = fetch(weight_pairs(weight_hbm, weight_ref, 0), sems)
    for copy in copies:
        copy.wait()
    for out_ref, d in zip(out_refs, hops):
        out_ref[...] = dot(gated_ref[...], weight_ref[d]).astype(bf16)


def finish_body(res_ref, conv_ref, skip_ref, key_ref, value_ref, gk_ref, gv_ref, gf_ref):
    local_rows = key_ref.shape[0]
    gf_ref[...] = res_ref[:, 1].reshape(-1, local_rows).T
    product_grad = res_ref[:, 0].reshape(-1, local_rows).T.astype(f32)
    product_grad = product_grad + skip_ref[...] * conv_ref[...].astype(f32)
    gk_ref[...] = (product_grad * value_ref[...].astype(f32)).astype(bf16)
    gv_ref[...] = (product_grad * key_ref[...].astype(f32)).astype(bf16)


def call(body, operands, results, scratch=(), flops=1 << 20, hbm=(), copies=0, limit=16):
    vmem = pl.BlockSpec(memory_space=pltpu.VMEM)
    left = pl.BlockSpec(memory_space=pltpu.HBM)
    scratch = list(scratch)
    if copies:
        scratch.append(pltpu.SemaphoreType.DMA((copies,)))
    kernel = pl.pallas_call(
        body,
        in_specs=[left if i in hbm else vmem for i in range(len(operands))],
        out_specs=[vmem] * len(results),
        out_shape=[jax.ShapeDtypeStruct(dims, kind) for dims, kind in results],
        scratch_shapes=scratch,
        cost_estimate=pl.CostEstimate(flops=flops, transcendentals=0, bytes_accessed=4 << 20),
        compiler_params=pltpu.CompilerParams(vmem_limit_bytes=limit << 20),
    )
    stay = pltpu.with_memory_space_constraint
    return list(kernel(*(stay(x, pltpu.HBM) if i in hbm else x for i, x in enumerate(operands))))


def to_all(x, axis):
    return lax.all_to_all(x, axis, split_axis=0, concat_axis=0, tiled=True)


def step(queries, key_in, value_in, filter_raw, skip_gain, out_weight, cotangent):
    local_rows, local_width = queries.shape
    seq_devices = lax.axis_size("seq")
    ch_devices = lax.axis_size("ch")
    length = local_rows * seq_devices
    width = local_width // seq_devices
    half = length // LANES
    first, over, under, last, turns = [jnp.asarray(t) for t in tables(length, seq_devices)]
    table = (first, turns, over, under, last)
    skip = skip_gain.reshape(1, local_width)
    message = (seq_devices, width, local_rows)
    pair = (seq_devices, 2, width, local_rows)
    flat = queries.shape
    near = ch_devices // 2
    work = [
        pltpu.VMEM((2, width, half, 2 * LANES), f32),
        pltpu.VMEM((local_rows // LANES, seq_devices * width, LANES), f32),
    ]
    own = pltpu.VMEM(flat, bf16)
    blocks = (near, local_width, local_width)

    def move(x, flip, shift):
        pairs = [(i, peer(i, near, flip, shift)) for i in range(ch_devices)]
        return lax.ppermute(x, "ch", pairs)

    hops = sorted(range(1, near), key=lambda d: -min(d, near - d))
    places = [0] + hops
    body = lambda f: functools.partial(f, places)

    other = move(cotangent, 1, 0)
    own_parts = [move(cotangent, 0, d) for d in hops]
    sent, pkv = call(
        prepare_body,
        (key_in, value_in, filter_raw),
        [(pair, bf16), (flat, bf16)],
        [own] * 3,
        hbm=(0, 1, 2),
        copies=3,
    )
    signals = to_all(sent, "seq")
    other_parts = [other] + [move(other, 0, d) for d in hops]

    mixed, *first_table = call(
        body(mixed_body),
        (out_weight, cotangent, *own_parts, *table[:3]),
        [(flat, f32)] + [(t.shape, t.dtype) for t in table[:3]],
        [own, pltpu.VMEM(blocks, bf16)],
        1 << 30,
        hbm=(0, 1, *range(1 + near, 4 + near)),
        copies=4 + near,
    )
    conv, spectra, far_weight, own_queries = call(
        conv_body,
        (signals, *first_table, *table[3:], out_weight, queries),
        [
            (message, bf16),
            ((2, width, half, 2 * LANES), f32),
            (blocks, bf16),
            (flat, bf16),
        ],
        work + [pltpu.VMEM(t.shape, t.dtype) for t in table[3:]],
        1 << 31,
        hbm=(4, 5, 6, 7),
        copies=near + 3,
    )
    mixed, grad_conv, both, *last_table = call(
        body(conv_grad_body),
        (far_weight, own_queries, mixed, conv, *other_parts, *table),
        [(flat, f32), (flat, bf16), (pair, bf16)] + [(t.shape, t.dtype) for t in table],
        flops=1 << 30,
        hbm=range(4 + near, 4 + near + len(table)),
        copies=len(table),
    )

    def moved(terms):
        out = []
        for k, d in enumerate(hops):
            out.append(move(terms[1 + k], 0, d))
        return out

    both = to_all(both, "seq")

    convolved, gated, *far_terms = call(
        body(gate_body),
        (far_weight, own_queries, both, pkv, skip),
        [(flat, f32), (flat, bf16)] + [(flat, bf16)] * near,
        flops=1 << 30,
    )
    far_terms = far_terms[:1] + moved(far_terms)
    near_terms = call(
        body(project_body),
        (out_weight, gated),
        [(flat, bf16)] * near,
        [pltpu.VMEM(blocks, bf16)],
        1 << 30,
        hbm=(0,),
        copies=near,
    )
    near_terms = near_terms[:1] + moved(near_terms)
    (results,) = call(
        back_body,
        (both, spectra, *last_table),
        [(pair, bf16)],
        work,
        1 << 31,
    )
    results = to_all(results, "seq")

    total = lambda terms: sum(x.astype(f32) for x in terms)
    across = move(total(far_terms).astype(bf16), 1, 0)
    grad_query = (mixed * convolved).astype(bf16)
    grad_key, grad_value, grad_filter = call(
        finish_body, (results, grad_conv, skip, key_in, value_in), [(flat, bf16)] * 3
    )
    projected = total(near_terms + [across]).astype(bf16)
    return (projected, grad_query, grad_key, grad_value, grad_filter)


def solution(mesh):
    placed = (
        P("seq", "ch"),
        P("seq", "ch"),
        P("seq", "ch"),
        P("seq", "ch"),
        P("ch"),
        P("ch", None),
        P("seq", "ch"),
    )
    return jax.shard_map(
        step,
        mesh=mesh,
        in_specs=placed,
        out_specs=(P("seq", "ch"),) * 5,
        check_vma=False,
    )
```

```python
import functools
import math

import jax
import jax.numpy as jnp
import numpy as np
from jax import lax
from jax.experimental import pallas as pl
from jax.experimental.pallas import tpu as pltpu
from jax.sharding import PartitionSpec as P


bf16 = jnp.bfloat16
f32 = jnp.float32
LANES = 128


def split(table):
    high = table.astype(bf16)
    low = (table - high.astype(np.float64)).astype(bf16)
    return np.asarray(high), np.asarray(low)


def tables(length, devices):
    points = 2 * length
    half = points // LANES // 2
    parts = half // devices
    rows = np.arange(half)
    j = parts * (rows % devices) + rows // devices
    k1 = np.arange(half) + 0.5
    lanes = np.arange(LANES)
    angle = 2.0 * np.pi / (2 * half) * np.outer(k1, j)
    first = np.concatenate([np.cos(angle), -np.sin(angle)], 0)
    last = np.concatenate([np.cos(angle.T), -np.sin(angle.T)], 1)
    turn = 2.0 * np.pi / points * np.outer(k1, lanes)
    factor = 2.0 / (points * math.sqrt(length))
    turns = np.stack([np.cos(turn), -np.sin(turn), np.cos(turn) * factor, np.sin(turn) * factor])
    phase = 2.0 * np.pi / LANES * (np.outer(lanes, lanes) % LANES)
    c, s = np.cos(phase), np.sin(phase)
    over = np.block([[c, -s], [s, c]])
    under = np.block([[c, s], [-s, c]])
    first_high, first_low = split(first)
    last_high, last_low = split(last)
    return (
        np.concatenate([first_high, first_low], 0),
        over.astype(bf16),
        under.astype(bf16),
        np.concatenate([last_high, last_low], 0),
        turns.astype(np.float32),
    )


def dot(a, b):
    return lax.dot_general(a, b, (((1,), (0,)), ((), ())), preferred_element_type=f32)


def forward(signals, first, turns):
    half = turns.shape[1]
    both = dot(first, jnp.concatenate(signals, 1))
    a = both[: 2 * half] + both[2 * half :]
    rotated = []
    for k in range(len(signals)):
        real = a[:half, k * LANES : (k + 1) * LANES]
        imag = a[half:, k * LANES : (k + 1) * LANES]
        pair = [real * turns[0] - imag * turns[1], real * turns[1] + imag * turns[0]]
        rotated.append(jnp.concatenate(pair, 1))
    return rotated


def lanes_dot(x, table):
    return dot(x.astype(bf16), table[...])


def backward(spectra, last, turns):
    turned = []
    for b in spectra:
        real, imag = b[:, :LANES], b[:, LANES:]
        pair = [real * turns[2] - imag * turns[3], real * turns[3] + imag * turns[2]]
        turned.append(jnp.concatenate(pair, 0).astype(bf16))
    rows = last.shape[0] // 2
    both = dot(last, jnp.concatenate(turned, 1))
    y = both[:rows] + both[rows:]
    return [y[:, k * LANES : (k + 1) * LANES] for k in range(len(spectra))]


def product(a, b, conjugate):
    ar, ai = a[:, :LANES], a[:, LANES:]
    br, bi = b[:, :LANES], b[:, LANES:]
    if conjugate:
        return jnp.concatenate([ar * br + ai * bi, ar * bi - ai * br], 1)
    return jnp.concatenate([ar * br - ai * bi, ar * bi + ai * br], 1)


def fetch(pairs, sems):
    copies = [pltpu.make_async_copy(a, b, sems.at[i]) for i, (a, b) in enumerate(pairs)]
    for copy in copies:
        copy.start()
    return copies


def prepare_body(key_hbm, value_hbm, filter_hbm, out_ref, pkv_ref, key_ref, value_ref, filter_ref, sems):
    copies = fetch([(filter_hbm, filter_ref), (key_hbm, key_ref), (value_hbm, value_ref)], sems)
    peers, _, width, local_rows = out_ref.shape
    copies[0].wait()
    out_ref[:, 1] = filter_ref[...].T.reshape(peers, width, local_rows)
    copies[1].wait()
    copies[2].wait()
    pkv = (key_ref[...].astype(f32) * value_ref[...].astype(f32)).astype(bf16)
    pkv_ref[...] = pkv
    out_ref[:, 0] = pkv.T.reshape(peers, width, local_rows)


def spread(x, rows_ref):
    for p in range(rows_ref.shape[0]):
        part = x[:, :, p * LANES : (p + 1) * LANES]
        rows_ref[p] = part.astype(f32).reshape(rows_ref.shape[1:])


def gather(rows_ref, out_ref, s):
    for p in range(rows_ref.shape[0]):
        part = rows_ref[p].reshape(*out_ref.shape[:1], *out_ref.shape[-2:-1], LANES).astype(bf16)
        if s is None:
            out_ref[:, :, p * LANES : (p + 1) * LANES] = part
        else:
            out_ref[:, s, :, p * LANES : (p + 1) * LANES] = part


def channel(rows_ref, c, devices, width):
    parts = [rows_ref[p, pl.ds(c, devices, stride=width), :] for p in range(rows_ref.shape[0])]
    return jnp.concatenate(parts, 0).astype(bf16)


def put_channel(rows_ref, c, devices, width, y):
    for p in range(rows_ref.shape[0]):
        rows_ref[p, pl.ds(c, devices, stride=width), :] = y[p * devices : (p + 1) * devices]


def conv_body(
    x_ref, first_ref, turns_ref, over_ref, under_hbm, last_hbm, weight_hbm, queries_hbm,
    out_ref, spec_ref, weight_ref, queries_ref, a_ref, rows_ref, under_ref, last_ref, sems,
):
    pairs = [(under_hbm, under_ref), (last_hbm, last_ref)]
    pairs += weight_pairs(weight_hbm, weight_ref, 1) + [(queries_hbm, queries_ref)]
    copies = fetch(pairs, sems)
    devices, _, width, _ = x_ref.shape
    half = turns_ref.shape[1]
    for s in range(2):
        spread(x_ref[:, s], rows_ref)
        for c in range(0, width, 2):
            x = [channel(rows_ref, c + k, devices, width) for k in range(2)]
            a_ref[s, c], a_ref[s, c + 1] = forward(x, first_ref[...], turns_ref)
    spectra = lanes_dot(a_ref[...].reshape(2 * width * half, 2 * LANES), over_ref)
    spec_ref[...] = spectra.reshape(spec_ref.shape)
    for c in range(width):
        a_ref[0, c] = product(spec_ref[1, c], spec_ref[0, c], False)
    copies[0].wait()
    copies[1].wait()
    b = lanes_dot(a_ref[0].reshape(width * half, 2 * LANES), under_ref)
    a_ref[1] = b.reshape(width, half, 2 * LANES)
    for c in range(0, width, 2):
        y = backward([a_ref[1, c], a_ref[1, c + 1]], last_ref[...], turns_ref)
        for k in range(2):
            put_channel(rows_ref, c + k, devices, width, y[k])
    gather(rows_ref, out_ref, None)
    for copy in copies[2:]:
        copy.wait()


def back_body(
    x_ref, spec_ref, first_ref, turns_ref, over_ref, under_ref, last_ref, out_ref, a_ref, rows_ref
):
    devices, _, width, _ = x_ref.shape
    half = turns_ref.shape[1]
    spread(x_ref[:, 1], rows_ref)
    for c in range(0, width, 2):
        x = [channel(rows_ref, c + k, devices, width) for k in range(2)]
        a_ref[0, c], a_ref[0, c + 1] = forward(x, first_ref[...], turns_ref)
    g = lanes_dot(a_ref[0].reshape(width * half, 2 * LANES), over_ref)
    a_ref[0] = g.reshape(width, half, 2 * LANES)
    for c in range(width):
        g_c = a_ref[0, c]
        a_ref[1, c] = product(spec_ref[0, c], g_c, True)
        a_ref[0, c] = product(spec_ref[1, c], g_c, True)
    b = lanes_dot(a_ref[...].reshape(2 * width * half, 2 * LANES), under_ref)
    a_ref[...] = b.reshape(a_ref.shape)
    for s in range(2):
        for c in range(0, width, 2):
            y = backward([a_ref[s, c], a_ref[s, c + 1]], last_ref[...], turns_ref)
            for k in range(2):
                put_channel(rows_ref, c + k, devices, width, y[k])
        gather(rows_ref, out_ref, s)


def peer(index, near, flip, shift):
    return (index // near + flip) % 2 * near + (index % near + shift) % near


def weight_pairs(weight_hbm, weight_ref, flip):
    here = lax.axis_index("ch")
    near, _, width = weight_ref.shape
    pairs = []
    for k in range(near):
        start = pl.multiple_of(peer(here, near, flip, k) * width, width)
        pairs.append((weight_hbm.at[:, pl.ds(start, width)], weight_ref.at[k]))
    return pairs


def mixed_term(part_ref, block):
    return lax.dot_general(
        part_ref[...], block, (((1,), (1,)), ((), ())), preferred_element_type=f32
    )


def mixed_body(hops, weight_hbm, own_hbm, *refs):
    near = len(hops)
    others = (len(refs) - near - 3) // 2
    parts = refs[: near - 1]
    others_hbm = refs[near - 1 : near - 1 + others]
    out_ref, *others_ref = refs[near - 1 + others : -3]
    own_ref, weight_ref, sems = refs[-3:]
    pairs = [(own_hbm, own_ref)] + weight_pairs(weight_hbm, weight_ref, 0)
    copies = fetch(pairs + list(zip(others_hbm, others_ref)), sems)
    for copy in copies[: 1 + near]:
        copy.wait()
    total = None
    for part_ref, d in zip((own_ref, *parts), hops):
        term = mixed_term(part_ref, weight_ref[-d % near])
        total = term if total is None else total + term
    out_ref[...] = total
    for copy in copies[1 + near :]:
        copy.wait()


def conv_grad_body(hops, weight_ref, queries_ref, before_ref, forward_ref, *refs):
    near = len(hops)
    others = (len(refs) - near - 4) // 2
    parts = refs[:near]
    others_hbm = refs[near : near + others]
    mixed_ref, conv_ref, sent_ref, *others_ref = refs[near + others : -1]
    copies = fetch(list(zip(others_hbm, others_ref)), refs[-1])
    sent_ref[:, 0] = forward_ref[...]
    mixed = before_ref[...]
    for part_ref, d in zip(parts, hops):
        mixed = mixed + mixed_term(part_ref, weight_ref[-d % near])
    mixed_ref[...] = mixed
    g = (mixed * queries_ref[...].astype(f32)).astype(bf16)
    conv_ref[...] = g
    sent_ref[:, 1] = g.T.reshape(forward_ref.shape)
    for copy in copies:
        copy.wait()


def gate_body(hops, weight_ref, queries_ref, conv_ref, pkv_ref, skip_ref, *refs):
    convolved_ref, gated_ref, *out_refs = refs
    local_rows = queries_ref.shape[0]
    conv = conv_ref[:, 0].reshape(-1, local_rows).T.astype(f32)
    convolved = conv + skip_ref[...] * pkv_ref[...].astype(f32)
    convolved_ref[...] = convolved
    gated = (queries_ref[...].astype(f32) * convolved).astype(bf16)
    gated_ref[...] = gated
    for out_ref, d in zip(out_refs, hops):
        out_ref[...] = dot(gated, weight_ref[d]).astype(bf16)


def project_body(hops, weight_hbm, gated_ref, *refs):
    *out_refs, weight_ref, sems = refs
    copies = fetch(weight_pairs(weight_hbm, weight_ref, 0), sems)
    for d in range(len(hops)):
        copies[d].wait()
        out_refs[hops.index(d)][...] = dot(gated_ref[...], weight_ref[d]).astype(bf16)


def finish_body(res_ref, conv_ref, skip_ref, key_ref, value_ref, gk_ref, gv_ref, gf_ref):
    local_rows = key_ref.shape[0]
    gf_ref[...] = res_ref[:, 1].reshape(-1, local_rows).T
    product_grad = res_ref[:, 0].reshape(-1, local_rows).T.astype(f32)
    product_grad = product_grad + skip_ref[...] * conv_ref[...].astype(f32)
    gk_ref[...] = (product_grad * value_ref[...].astype(f32)).astype(bf16)
    gv_ref[...] = (product_grad * key_ref[...].astype(f32)).astype(bf16)


def call(body, operands, results, scratch=(), flops=1 << 20, hbm=(), copies=0, limit=16):
    vmem = pl.BlockSpec(memory_space=pltpu.VMEM)
    left = pl.BlockSpec(memory_space=pltpu.HBM)
    scratch = list(scratch)
    if copies:
        scratch.append(pltpu.SemaphoreType.DMA((copies,)))
    kernel = pl.pallas_call(
        body,
        in_specs=[left if i in hbm else vmem for i in range(len(operands))],
        out_specs=[vmem] * len(results),
        out_shape=[jax.ShapeDtypeStruct(dims, kind) for dims, kind in results],
        scratch_shapes=scratch,
        cost_estimate=pl.CostEstimate(flops=flops, transcendentals=0, bytes_accessed=4 << 20),
        compiler_params=pltpu.CompilerParams(vmem_limit_bytes=limit << 20),
    )
    stay = pltpu.with_memory_space_constraint
    return list(kernel(*(stay(x, pltpu.HBM) if i in hbm else x for i, x in enumerate(operands))))


def to_all(x, axis):
    return lax.all_to_all(x, axis, split_axis=0, concat_axis=0, tiled=True)


def step(queries, key_in, value_in, filter_raw, skip_gain, out_weight, cotangent):
    local_rows, local_width = queries.shape
    seq_devices = lax.axis_size("seq")
    ch_devices = lax.axis_size("ch")
    length = local_rows * seq_devices
    width = local_width // seq_devices
    half = length // LANES
    first, over, under, last, turns = [jnp.asarray(t) for t in tables(length, seq_devices)]
    table = (first, turns, over, under, last)
    skip = skip_gain.reshape(1, local_width)
    message = (seq_devices, width, local_rows)
    pair = (seq_devices, 2, width, local_rows)
    flat = queries.shape
    near = ch_devices // 2
    work = [
        pltpu.VMEM((2, width, half, 2 * LANES), f32),
        pltpu.VMEM((local_rows // LANES, seq_devices * width, LANES), f32),
    ]
    own = pltpu.VMEM(flat, bf16)
    blocks = (near, local_width, local_width)

    def move(x, flip, shift):
        pairs = [(i, peer(i, near, flip, shift)) for i in range(ch_devices)]
        return lax.ppermute(x, "ch", pairs)

    hops = sorted(range(1, near), key=lambda d: -min(d, near - d))
    places = [0] + hops
    body = lambda f: functools.partial(f, places)

    other = move(cotangent, 1, 0)
    own_parts = [move(cotangent, 0, d) for d in hops]
    sent, pkv = call(
        prepare_body,
        (key_in, value_in, filter_raw),
        [(pair, bf16), (flat, bf16)],
        [own] * 3,
        hbm=(0, 1, 2),
        copies=3,
    )
    signals = to_all(sent, "seq")
    other_parts = [other] + [move(other, 0, d) for d in hops]

    mixed, *first_table = call(
        body(mixed_body),
        (out_weight, cotangent, *own_parts, *table[:3]),
        [(flat, f32)] + [(t.shape, t.dtype) for t in table[:3]],
        [own, pltpu.VMEM(blocks, bf16)],
        1 << 30,
        hbm=(0, 1, *range(1 + near, 4 + near)),
        copies=4 + near,
    )
    conv, spectra, far_weight, own_queries = call(
        conv_body,
        (signals, *first_table, *table[3:], out_weight, queries),
        [
            (message, bf16),
            ((2, width, half, 2 * LANES), f32),
            (blocks, bf16),
            (flat, bf16),
        ],
        work + [pltpu.VMEM(t.shape, t.dtype) for t in table[3:]],
        1 << 31,
        hbm=(4, 5, 6, 7),
        copies=near + 3,
    )
    mixed, grad_conv, both, *last_table = call(
        body(conv_grad_body),
        (far_weight, own_queries, mixed, conv, *other_parts, *table),
        [(flat, f32), (flat, bf16), (pair, bf16)] + [(t.shape, t.dtype) for t in table],
        flops=1 << 30,
        hbm=range(4 + near, 4 + near + len(table)),
        copies=len(table),
    )

    def moved(terms):
        out = []
        for k, d in enumerate(hops):
            out.append(move(terms[1 + k], 0, d))
        return out

    both = to_all(both, "seq")

    convolved, gated, *far_terms = call(
        body(gate_body),
        (far_weight, own_queries, both, pkv, skip),
        [(flat, f32), (flat, bf16)] + [(flat, bf16)] * near,
        flops=1 << 30,
    )
    far_terms = far_terms[:1] + moved(far_terms)
    near_terms = call(
        body(project_body),
        (out_weight, gated),
        [(flat, bf16)] * near,
        [pltpu.VMEM(blocks, bf16)],
        1 << 30,
        hbm=(0,),
        copies=near,
    )
    near_terms = near_terms[:1] + moved(near_terms)
    (results,) = call(
        back_body,
        (both, spectra, *last_table),
        [(pair, bf16)],
        work,
        1 << 31,
    )
    results = to_all(results, "seq")

    total = lambda terms: sum(x.astype(f32) for x in terms)
    across = move(total(far_terms).astype(bf16), 1, 0)
    grad_query = (mixed * convolved).astype(bf16)
    grad_key, grad_value, grad_filter = call(
        finish_body, (results, grad_conv, skip, key_in, value_in), [(flat, bf16)] * 3
    )
    projected = total(near_terms + [across]).astype(bf16)
    return (projected, grad_query, grad_key, grad_value, grad_filter)


def solution(mesh):
    placed = (
        P("seq", "ch"),
        P("seq", "ch"),
        P("seq", "ch"),
        P("seq", "ch"),
        P("ch"),
        P("ch", None),
        P("seq", "ch"),
    )
    return jax.shard_map(
        step,
        mesh=mesh,
        in_specs=placed,
        out_specs=(P("seq", "ch"),) * 5,
        check_vma=False,
    )
```
